128 devices in a mesh: dp: 1, sp: 128 (over z, y, x, core).
Axes of the slice: x: 4, y: 4, z: 4, core: 2. Of those that a mesh axis runs over, the one named last changes fastest.
Arguments:
- pair_rep: float32 [768, 768, 128], P(('dp', 'sp'))
- w_qkvg_s: bfloat16 [128, 512], replicated
- w_bias_s: bfloat16 [4, 128], replicated
- w_out_s: bfloat16 [128, 128], replicated
- w_qkvg_e: bfloat16 [128, 512], replicated
- w_bias_e: bfloat16 [4, 128], replicated
- w_out_e: bfloat16 [128, 128], replicated
- w_one: bfloat16 [128, 512], replicated
- w_two: bfloat16 [512, 128], replicated
Outputs:
- output: float32 [768, 768, 128], P(('dp', 'sp'))
All inputs are finite; a program needn't handle non-finite values.
Results may differ from the reference program's by a relative error of at most 0.0108011.
Values are sent between devices in bfloat16 or wider.
A program may use at most 1 GiB of HBM per device.

```python
import jax
import jax.numpy as jnp
from jax import lax

N = 768
C_Z = 128
HEADS = 4
HEAD_DIM = C_Z // HEADS
HIDDEN = 4 * C_Z
LN_EPS = 1e-5
OUT_SCALE = (N / 16) ** 0.5


def setup_inputs(seed: int = 0, part: int = 0) -> dict:
    root_key = jax.random.key(seed)
    part_key = jax.random.fold_in(root_key, part)
    shared = jax.random.split(jax.random.fold_in(root_key, 65537), 8)
    in_scale = C_Z ** -0.5
    hid_scale = HIDDEN ** -0.5
    pair_rep = jax.random.normal(part_key, (N, N, C_Z), jnp.float32)
    w_qkvg_s = jax.random.normal(shared[0], (C_Z, 4 * C_Z), jnp.float32) * in_scale
    w_bias_s = jax.random.normal(shared[1], (HEADS, C_Z), jnp.float32) * in_scale
    w_out_s = jax.random.normal(shared[2], (C_Z, C_Z), jnp.float32) * (in_scale * OUT_SCALE)
    w_qkvg_e = jax.random.normal(shared[3], (C_Z, 4 * C_Z), jnp.float32) * in_scale
    w_bias_e = jax.random.normal(shared[4], (HEADS, C_Z), jnp.float32) * in_scale
    w_out_e = jax.random.normal(shared[5], (C_Z, C_Z), jnp.float32) * (in_scale * OUT_SCALE)
    w_one = jax.random.normal(shared[6], (C_Z, HIDDEN), jnp.float32) * in_scale
    w_two = jax.random.normal(shared[7], (HIDDEN, C_Z), jnp.float32) * hid_scale
    return {
        "pair_rep": pair_rep,
        "w_qkvg_s": w_qkvg_s.astype(jnp.bfloat16),
        "w_bias_s": w_bias_s.astype(jnp.bfloat16),
        "w_out_s": w_out_s.astype(jnp.bfloat16),
        "w_qkvg_e": w_qkvg_e.astype(jnp.bfloat16),
        "w_bias_e": w_bias_e.astype(jnp.bfloat16),
        "w_out_e": w_out_e.astype(jnp.bfloat16),
        "w_one": w_one.astype(jnp.bfloat16),
        "w_two": w_two.astype(jnp.bfloat16),
    }


def layer_norm(values):
    vals_f = values.astype(jnp.float32)
    mean_c = jnp.mean(vals_f, axis=-1, keepdims=True)
    centered = vals_f - mean_c
    variance = jnp.mean(centered * centered, axis=-1, keepdims=True)
    return (centered * lax.rsqrt(variance + LN_EPS)).astype(jnp.bfloat16)


def bias_table(pair_in, w_bias):
    def one_row(row_in):
        return jnp.dot(layer_norm(row_in), w_bias.T, preferred_element_type=jnp.float32).astype(jnp.bfloat16)
    return jnp.transpose(lax.map(one_row, pair_in), (2, 0, 1))


def row_update(row_in, bias_full, w_qkvg, w_out):
    seq_len = row_in.shape[0]
    projected = jnp.dot(layer_norm(row_in), w_qkvg, preferred_element_type=jnp.float32)
    split_shape = (seq_len, HEADS, HEAD_DIM)
    queries = projected[:, :C_Z].astype(jnp.bfloat16).reshape(split_shape).astype(jnp.float32)
    key_vecs = projected[:, C_Z:2 * C_Z].astype(jnp.bfloat16).reshape(split_shape).astype(jnp.float32)
    val_vecs = projected[:, 2 * C_Z:3 * C_Z].astype(jnp.bfloat16).reshape(split_shape).astype(jnp.float32)
    gate_vals = jax.nn.sigmoid(projected[:, 3 * C_Z:]).reshape(split_shape)
    scores = jnp.einsum('jhd,khd->hjk', queries, key_vecs) * HEAD_DIM ** -0.5 + bias_full.astype(jnp.float32)
    attn_prob = jax.nn.softmax(scores, axis=-1).astype(jnp.bfloat16).astype(jnp.float32)
    attn_out = jnp.einsum('hjk,khd->jhd', attn_prob, val_vecs)
    gated_out = (attn_out * gate_vals).astype(jnp.bfloat16).reshape(seq_len, C_Z)
    return jnp.dot(gated_out, w_out, preferred_element_type=jnp.float32)


def tri_attention(pair_in, w_qkvg, w_bias, w_out):
    bias_full = bias_table(pair_in, w_bias)

    def one_row(row_in):
        return row_update(row_in, bias_full, w_qkvg, w_out)
    return lax.map(one_row, pair_in)


def reference(pair_rep, w_qkvg_s, w_bias_s, w_out_s, w_qkvg_e, w_bias_e, w_out_e, w_one, w_two):
    pair_one = pair_rep + tri_attention(pair_rep, w_qkvg_s, w_bias_s, w_out_s)
    pair_trans = jnp.swapaxes(pair_one.astype(jnp.bfloat16), 0, 1)
    end_upd = tri_attention(pair_trans, w_qkvg_e, w_bias_e, w_out_e)

    def finish_row(row_pair):
        trans_row, upd_row = row_pair
        pair_two = trans_row.astype(jnp.float32) + upd_row
        hidden = jax.nn.relu(jnp.dot(layer_norm(pair_two), w_one, preferred_element_type=jnp.float32))
        trans_out = jnp.dot(hidden.astype(jnp.bfloat16), w_two, preferred_element_type=jnp.float32)
        return (upd_row + trans_out).astype(jnp.bfloat16)

    delta_trans = lax.map(finish_row, (pair_trans, end_upd))
    return pair_one + jnp.swapaxes(delta_trans, 0, 1).astype(jnp.float32)
```

```python
import functools
import math
import jax
import jax.numpy as jnp
from jax import lax
from jax.experimental import pallas as pl
from jax.experimental.pallas import tpu as pltpu
from jax.sharding import PartitionSpec as P

F32, BF16 = jnp.float32, jnp.bfloat16
LOG2E = math.log2(math.e)
EPS = 1e-5

def ln(x):
    mu = jnp.mean(x, axis=-1, keepdims=True)
    c = x - mu
    var = jnp.mean(c * c, axis=-1, keepdims=True)
    return (c * lax.rsqrt(var + EPS)).astype(BF16)

def dotf(a, b):
    return jnp.dot(a, b, preferred_element_type=F32)

def dot_nt(a, b):
    return lax.dot_general(a, b, (((1,), (1,)), ((), ())), preferred_element_type=F32)

def attn_kernel(end, n, heads, nq, x_ref, bias_ref, wqvg_ref, wkT_ref, wo_ref, w1_ref, w2_ref, o_ref, bf_ref, q_ref, g_ref, kT_ref, v_ref, s_ref):
    c = x_ref.shape[-1]
    hd = c // heads
    @pl.when(pl.program_id(0) == 0)
    def _():
        for h in range(heads):
            def cvt(r, _):
                rows = pl.ds(pl.multiple_of(r * 64, 64), 64)
                bf_ref[h, rows, :] = bias_ref[h, rows, :].astype(F32) * LOG2E
                return 0
            lax.fori_loop(0, n // 64, cvt, 0)
        v_ref[:, c:] = jnp.ones((n, c), BF16)
    x = x_ref[0].astype(F32)
    u = ln(x)
    kT_ref[...] = dot_nt(wkT_ref[...], u).astype(BF16)
    pr = dotf(u, wqvg_ref[...])
    q_ref[...] = pr[:, :c].astype(BF16)
    v_ref[:, :c] = pr[:, c:2 * c].astype(BF16)
    g_ref[...] = jax.nn.sigmoid(pr[:, 2 * c:])
    scale = hd ** -0.5 * LOG2E
    def block(b, _):
        rows = pl.ds(pl.multiple_of(b * nq, nq), nq)
        qb = q_ref[rows, :]
        lane = lax.broadcasted_iota(jnp.int32, (nq, c), 1) // hd
        res = jnp.zeros((nq, c), F32)
        for h in range(heads):
            qm = jnp.where(lane == h, qb, jnp.zeros_like(qb))
            s = dotf(qm, kT_ref[...])
            t = s * scale + bf_ref[h, rows, :]
            m = jnp.max(t, axis=-1, keepdims=True)
            p = jnp.exp2(t - m).astype(BF16)
            o = dotf(p, v_ref[...])
            res = jnp.where(lane == h, o[:, :c] / o[:, c:], res)
        og = (res * g_ref[rows, :]).astype(BF16)
        upd = dotf(og, wo_ref[...])
        if not end:
            o_ref[0, rows, :] = x_ref[0, rows, :] + upd
        else:
            two = x_ref[0, rows, :].astype(F32) + upd
            hid = jnp.maximum(dotf(ln(two), w1_ref[...]), 0).astype(BF16)
            o_ref[0, rows, :] = (upd + dotf(hid, w2_ref[...])).astype(BF16)
        return 0
    lax.fori_loop(0, n // nq, block, 0)

def attention(x, bias, wqkvg, wo, w1, w2, end, nq=384):
    rows, n, c = x.shape
    heads = bias.shape[0]
    wqvg = jnp.concatenate([wqkvg[:, :c], wqkvg[:, 2 * c:]], axis=1)
    wkT = wqkvg[:, c:2 * c].T
    full = lambda a: pl.BlockSpec(a.shape, lambda i: (0,) * a.ndim, pipeline_mode=pl.Buffered(1))
    return pl.pallas_call(
        functools.partial(attn_kernel, end, n, heads, nq),
        grid=(rows,),
        in_specs=[pl.BlockSpec((1, n, c), lambda i: (i, 0, 0)), full(bias), full(wqvg), full(wkT), full(wo), full(w1), full(w2)],
        out_specs=pl.BlockSpec((1, n, c), lambda i: (i, 0, 0)),
        out_shape=jax.ShapeDtypeStruct((rows, n, c), BF16 if end else F32),
        scratch_shapes=[pltpu.VMEM((heads, n, n), F32), pltpu.VMEM((n, c), BF16), pltpu.VMEM((n, c), F32), pltpu.VMEM((c, n), BF16), pltpu.VMEM((n, 2 * c), BF16), pltpu.VMEM((8, 128), F32)],
        compiler_params=pltpu.CompilerParams(vmem_limit_bytes=60 * 2**20),
    )(x, bias, wqvg, wkT, wo, w1, w2)


def solution(mesh):
    row_spec = P(('dp', 'sp'), None, None)

    def local_fn(z, wqkvg_s, wb_s, wo_s, wqkvg_e, wb_e, wo_e, w1, w2):
        bias_s = jnp.einsum('hc,jkc->hjk', wb_s, ln(z), preferred_element_type=F32).astype(BF16)
        bias_s = lax.all_gather(bias_s, 'sp', axis=1, tiled=True)
        z1 = attention(z, bias_s, wqkvg_s, wo_s, w1, w2, False)
        cols = lax.all_to_all(z1.astype(BF16), 'sp', 1, 0, tiled=True)
        cols = jnp.swapaxes(cols, 0, 1)
        bias_e = jnp.einsum('hc,ikc->hik', wb_e, ln(cols.astype(F32)), preferred_element_type=F32).astype(BF16)
        bias_e = lax.all_gather(bias_e, 'sp', axis=1, tiled=True)
        delta = attention(cols, bias_e, wqkvg_e, wo_e, w1, w2, True)
        delta = lax.all_to_all(jnp.swapaxes(delta, 0, 1), 'sp', 0, 1, tiled=True)
        return z1 + delta.astype(F32)

    return jax.shard_map(local_fn, mesh=mesh, in_specs=(row_spec,) + (P(),) * 8, out_specs=row_spec, check_vma=False)
```

```python
import functools
import math
import random
import jax
import jax.numpy as jnp
import numpy as np
from jax import lax
from jax.experimental import pallas as pl
from jax.experimental.pallas import tpu as pltpu
from jax.sharding import PartitionSpec as P

F32, BF16 = jnp.float32, jnp.bfloat16
LOG2E = math.log2(math.e)
EPS = 1e-5
MESH = pl.DeviceIdType.MESH
STRIDES = (2, 8, 32)

def rcopy(src, dst, ssem, rsem, peer):
    return pltpu.make_async_remote_copy(src_ref=src, dst_ref=dst, send_sem=ssem, recv_sem=rsem, device_id={'sp': peer}, device_id_type=MESH)

def bytes_wait(ref, sem):
    pltpu.make_async_copy(ref, ref, sem).wait()

def coord(me, s):
    return lax.rem(me // s, 4)

def ring(me, s, t):
    cc = coord(me, s)
    return me + (lax.rem(cc + t, 4) - cc) * s

def gather_start(me, x_ref, o_ref, ssem, rsem):
    for c in range(3):
        sa = STRIDES[c]
        for t in (1, 3, 2):
            rcopy(x_ref.at[c], o_ref.at[c, me], ssem, rsem.at[c, 0], ring(me, sa, t)).start()
        rcopy(x_ref.at[c], o_ref.at[c, me], ssem, rsem.at[c, 5], me ^ 1).start()

def gather_rest(me, x_ref, o_ref, ssem, rsem):
    dims = [(STRIDES[c], STRIDES[(c + 1) % 3], STRIDES[(c + 2) % 3]) for c in range(3)]
    def push(c, d, peer, k):
        rcopy(o_ref.at[c, d], o_ref.at[c, d], ssem, rsem.at[c, k], peer).start()
    partner = me ^ 1
    for c in range(3):
        sa, sb, sd = dims[c]
        bytes_wait(o_ref.at[c, pl.ds(0, 3)], rsem.at[c, 0])
        base = me - coord(me, sa) * sa
        def body(j, _):
            d = base + j * sa
            for t in (1, 3, 2):
                push(c, d, ring(me, sb, t), 1)
            @pl.when(d != me)
            def _():
                push(c, d, partner, 5)
            return 0
        lax.fori_loop(0, 4, body, 0)
    for c in range(3):
        sa, sb, sd = dims[c]
        bytes_wait(o_ref.at[c, pl.ds(0, 12)], rsem.at[c, 1])
        cb = coord(me, sb)
        base = me - coord(me, sa) * sa - cb * sb
        def body(j, _):
            jb = j // 4
            d = base + lax.rem(j, 4) * sa + jb * sb
            push(c, d, ring(me, sd, 1), 2)
            push(c, d, ring(me, sd, 3), 3)
            @pl.when(jb != cb)
            def _():
                push(c, d, partner, 5)
            return 0
        lax.fori_loop(0, 16, body, 0)
    for side in range(2):
        for c in range(3):
            sa, sb, sd = dims[c]
            bytes_wait(o_ref.at[c, pl.ds(0, 16)], rsem.at[c, 2 + side])
            src = ring(me, sd, 3 if side == 0 else 1)
            base = src - coord(me, sa) * sa - coord(me, sb) * sb
            to = ring(me, sd, 1 if side == 0 else 3)
            def body(j, _):
                d = base + lax.rem(j, 4) * sa + (j // 4) * sb
                @pl.when(j // 8 == side)
                def _():
                    push(c, d, to, 4)
                push(c, d, partner, 5)
                return 0
            lax.fori_loop(0, 16, body, 0)
    for c in range(3):
        sa, sb, sd = dims[c]
        bytes_wait(o_ref.at[c, pl.ds(0, 16)], rsem.at[c, 4])
        src = ring(me, sd, 2)
        base = src - coord(me, sa) * sa - coord(me, sb) * sb
        def body(j, _):
            push(c, base + lax.rem(j, 4) * sa + (j // 4) * sb, partner, 5)
            return 0
        lax.fori_loop(0, 16, body, 0)
    for c in range(3):
        bytes_wait(o_ref.at[c, pl.ds(0, 64)], rsem.at[c, 5])
    for c in range(3):
        bytes_wait(o_ref.at[c, pl.ds(0, 127)], ssem)

def exchange_start(me, h_ref, r_ref, n, ssem, rsem):
    for k in send_order(n):
        d = me ^ k
        rcopy(h_ref.at[d], r_ref.at[me], ssem, rsem, d).start()

def exchange_wait(r_ref, n, ssem, rsem):
    bytes_wait(r_ref.at[pl.ds(0, n - 1)], rsem)
    bytes_wait(r_ref.at[pl.ds(0, n - 1)], ssem)

def a2a_kernel(n, h_ref, r_ref, lsem, ssem, rsem):
    me = lax.axis_index('sp')
    own = pltpu.make_async_copy(h_ref.at[me], r_ref.at[me], lsem)
    own.start()
    exchange_start(me, h_ref, r_ref, n, ssem, rsem)
    own.wait()
    exchange_wait(r_ref, n, ssem, rsem)

def all_to_all(h, n):
    anyspec = pl.BlockSpec(memory_space=pl.ANY)
    return pl.pallas_call(functools.partial(a2a_kernel, n), in_specs=[anyspec], out_specs=anyspec,
        out_shape=jax.ShapeDtypeStruct(h.shape, h.dtype),
        scratch_shapes=[pltpu.SemaphoreType.DMA, pltpu.SemaphoreType.DMA, pltpu.SemaphoreType.DMA],
        compiler_params=pltpu.CompilerParams(has_side_effects=True), name='exchange')(h)


def send_order(n):
    groups = {}
    for k in range(1, n):
        x, y, z = (k >> 1) & 3, (k >> 3) & 3, (k >> 5) & 3
        g = (0, x) if x else (1, y) if y else (2, z)
        groups.setdefault(g, []).append(k)
    slots = []
    for ks in groups.values():
        ks = sorted(ks, key=lambda k: random.Random(k).random())
        slots += [((i + 0.5) / len(ks), k) for i, k in enumerate(ks)]
    return [k for _, k in sorted(slots)]


def ln(x):
    mu = jnp.mean(x, axis=-1, keepdims=True)
    c = x - mu
    var = jnp.mean(c * c, axis=-1, keepdims=True)
    return (c * lax.rsqrt(var + EPS)).astype(BF16)


def dotf(a, b):
    return jnp.dot(a, b, preferred_element_type=F32)


def dot_nt(a, b):
    return lax.dot_general(a, b, (((1,), (1,)), ((), ())), preferred_element_type=F32)


def pack_matrix(per, pad, devs):
    m = np.zeros((devs, pad, per, devs, per), np.float32)
    for d in range(devs):
        for a in range(per):
            for b in range(per):
                m[d, a * per + b, a, d, b] = 1
    return jnp.asarray(m.reshape(devs * pad, per * devs * per), BF16)


def unpack_matrix(per, pad, devs):
    m = np.zeros((per, devs, per, devs, pad), np.float32)
    for d in range(devs):
        for a in range(per):
            for b in range(per):
                m[b, d, a, d, a * per + b] = 1
    return jnp.asarray(m.reshape(per * devs * per, devs * pad), BF16)


def bias_matrix(per, heads, devs):
    m = np.zeros((heads, devs, per, devs, per, heads), np.float32)
    for d in range(devs):
        for a in range(per):
            for h in range(heads):
                m[h, d, a, d, a, h] = 1
    return jnp.asarray(m.reshape(heads * devs * per, devs * per * heads), BF16)


def pack_rows(src_ref, pm_ref, out_ref, devs):
    per, n, c = src_ref.shape
    pad = out_ref.shape[1]
    span = devs * per

    def body(g, _):
        rows = pl.ds(pl.multiple_of(g * span, span), span)
        x = jnp.concatenate([src_ref[a, rows, :] for a in range(per)], axis=0).astype(BF16)
        y = dotf(pm_ref[...], x).reshape(devs, pad, c).astype(BF16)
        out_ref[pl.ds(pl.multiple_of(g * devs, devs), devs)] = y
        return 0
    lax.fori_loop(0, n // span, body, 0)


def unpack_rows(r_ref, pm_ref, store, devs, per, n):
    pad, c = r_ref.shape[1:]
    span = devs * per

    def body(g, _):
        x = r_ref[pl.ds(pl.multiple_of(g * devs, devs), devs)].reshape(devs * pad, c)
        y = dotf(pm_ref[...], x)
        rows = pl.ds(pl.multiple_of(g * span, span), span)
        for b in range(per):
            store(b, rows, y[b * span:(b + 1) * span])
        return 0
    lax.fori_loop(0, n // span, body, 0)


def local_bias(x_ref, wr_ref, b_ref):
    per = x_ref.shape[0]
    acc = None
    for r in range(per):
        t = dot_nt(wr_ref[r], ln(x_ref[r].astype(F32)))
        acc = t if acc is None else acc + t
    acc = acc.astype(BF16)
    for c in range(3):
        b_ref[c] = acc[:, c * b_ref.shape[2]:(c + 1) * b_ref.shape[2]]


def start_gather_kernel(x_ref, wr_ref, o_ref, b_ref, lsem, ssem, rsem):
    me = lax.axis_index('sp')
    local_bias(x_ref, wr_ref, b_ref)
    own = pltpu.make_async_copy(b_ref, o_ref.at[:, me], lsem)
    own.start()
    gather_start(me, b_ref, o_ref, ssem, rsem)
    own.wait()
    gather_rest(me, b_ref, o_ref, ssem, rsem)


def end_gather_kernel(n, devs, h_ref, pm_ref, wr_ref, x_ref, o_ref, r_ref, b_ref, lsem, ssem, rsem, esem):
    me = lax.axis_index('sp')
    own = pltpu.make_async_copy(h_ref.at[me], r_ref.at[me], lsem)
    own.start()
    exchange_start(me, h_ref, r_ref, n, ssem, esem)
    own.wait()
    exchange_wait(r_ref, n, ssem, esem)

    def store(b, rows, y):
        x_ref[b, rows, :] = y
    unpack_rows(r_ref, pm_ref, store, devs, x_ref.shape[0], x_ref.shape[1])
    local_bias(x_ref, wr_ref, b_ref)
    own = pltpu.make_async_copy(b_ref, o_ref.at[:, me], lsem)
    own.start()
    gather_start(me, b_ref, o_ref, ssem, rsem)
    own.wait()
    gather_rest(me, b_ref, o_ref, ssem, rsem)


def finish_kernel(devs, r_ref, pm_ref, z_ref, y_ref):
    def store(b, rows, y):
        y_ref[b, rows, :] = z_ref[b, rows, :] + y
    unpack_rows(r_ref, pm_ref, store, devs, z_ref.shape[0], z_ref.shape[1])


def attn_kernel(end, heads, nq, bdevs, pdevs, x_ref, gb_ref, wqvg_ref, wkT_ref, wo_ref, w1_ref, w2_ref, bm_ref, pm_ref, *refs):
    if end:
        o_ref = None
        h_ref, bf_ref, q_ref, g_ref, kT_ref, v_ref, hs_ref = refs
    else:
        o_ref, h_ref, bf_ref, q_ref, g_ref, kT_ref, v_ref, hs_ref = refs
    n, c = x_ref.shape[1:]
    hd = c // heads
    i = pl.program_id(0)

    @pl.when(i == 0)
    def _():
        wid = gb_ref.shape[3]
        span = n // (gb_ref.shape[1] // bdevs)

        def unpack(g, _):
            rows = pl.ds(pl.multiple_of(g * span, span), span)
            for s in range(3):
                b = gb_ref[s, pl.ds(pl.multiple_of(g * bdevs, bdevs), bdevs)].reshape(heads * span, wid)
                f = dotf(bm_ref[...], b) * LOG2E
                for h in range(heads):
                    bf_ref[h, rows, s * wid:(s + 1) * wid] = f[h * span:(h + 1) * span]
            return 0
        lax.fori_loop(0, n // span, unpack, 0)
        v_ref[:, c:] = jnp.ones((n, c), BF16)

    u = ln(x_ref[0].astype(F32))
    kT_ref[...] = dot_nt(wkT_ref[...], u).astype(BF16)
    pr = dotf(u, wqvg_ref[...])
    q_ref[...] = pr[:, :c].astype(BF16)
    v_ref[:, :c] = pr[:, c:2 * c].astype(BF16)
    g_ref[...] = jax.nn.sigmoid(pr[:, 2 * c:])
    scale = hd ** -0.5 * LOG2E

    def block(b, _):
        rows = pl.ds(pl.multiple_of(b * nq, nq), nq)
        qb = q_ref[rows, :]
        lane = lax.broadcasted_iota(jnp.int32, (nq, c), 1) // hd
        res = jnp.zeros((nq, c), F32)
        for h in range(heads):
            qm = jnp.where(lane == h, qb, jnp.zeros_like(qb))
            s = dotf(qm, kT_ref[...])
            t = s * scale + bf_ref[h, rows, :]
            m = jnp.max(t, axis=-1, keepdims=True)
            p = jnp.exp2(t - m).astype(BF16)
            o = dotf(p, v_ref[...])
            res = jnp.where(lane == h, o[:, :c] / o[:, c:], res)
        og = (res * g_ref[rows, :]).astype(BF16)
        upd = dotf(og, wo_ref[...])
        two = x_ref[0, rows, :].astype(F32) + upd
        if end:
            hid = jnp.maximum(dotf(ln(two), w1_ref[...]), 0).astype(BF16)
            hs_ref[i, rows, :] = upd + dotf(hid, w2_ref[...])
        else:
            o_ref[0, rows, :] = two
            hs_ref[i, rows, :] = two
        return 0
    lax.fori_loop(0, n // nq, block, 0)

    @pl.when(i == pl.num_programs(0) - 1)
    def _():
        pack_rows(hs_ref, pm_ref, h_ref, pdevs)


def attention(x, gb, wqkvg, wo, w1, w2, bm, pm, end, heads, bdevs, pdevs, nq):
    per, n, c = x.shape
    devs = gb.shape[1]
    pad = pm.shape[0] // pdevs
    wqvg = jnp.concatenate([wqkvg[:, :c], wqkvg[:, 2 * c:]], axis=1)
    wkT = wqkvg[:, c:2 * c].T
    full = lambda a: pl.BlockSpec(a.shape, lambda i: (0,) * a.ndim, pipeline_mode=pl.Buffered(1))
    row = pl.BlockSpec((1, n, c), lambda i: (i, 0, 0))
    packed = jax.ShapeDtypeStruct((devs, pad, c), BF16)
    outs = [] if end else [(row, jax.ShapeDtypeStruct((per, n, c), F32))]
    outs.append((full(packed), packed))
    return pl.pallas_call(
        functools.partial(attn_kernel, end, heads, nq, bdevs, pdevs),
        grid=(per,),
        in_specs=[row] + [full(a) for a in (gb, wqvg, wkT, wo, w1, w2, bm, pm)],
        out_specs=[o[0] for o in outs],
        out_shape=[o[1] for o in outs],
        scratch_shapes=[pltpu.VMEM((heads, n, n), F32), pltpu.VMEM((n, c), BF16), pltpu.VMEM((n, c), F32),
                        pltpu.VMEM((c, n), BF16), pltpu.VMEM((n, 2 * c), BF16), pltpu.VMEM((per, n, c), F32)],
        compiler_params=pltpu.CompilerParams(vmem_limit_bytes=56 * 2**20),
        name='attend_end' if end else 'attend_start',
    )(x, gb, wqvg, wkT, wo, w1, w2, bm, pm)


def solution(mesh):
    devs = mesh.shape['sp']
    row_spec = P(('dp', 'sp'), None, None)
    vmem = pl.BlockSpec(memory_space=pltpu.VMEM)
    hbm = pl.BlockSpec(memory_space=pl.ANY)
    params = pltpu.CompilerParams(has_side_effects=True, vmem_limit_bytes=32 * 2**20)
    dma = pltpu.SemaphoreType.DMA

    def local_fn(z, wqkvg_s, wb_s, wo_s, wqkvg_e, wb_e, wo_e, w1, w2):
        per, n, c = z.shape
        heads = wb_s.shape[0]
        bdevs, pdevs = 8, 4
        pad = -(-per * per // 8) * 8
        wid = n // 3
        nb = per * heads
        eye = jnp.eye(per, dtype=BF16)
        expand = lambda wb: (eye[:, :, None, None] * wb[None, None]).reshape(per, nb, c)
        bm = bias_matrix(per, heads, bdevs)
        pm = pack_matrix(per, pad, pdevs)
        um = unpack_matrix(per, pad, pdevs)
        gathered = jax.ShapeDtypeStruct((3, devs, nb, wid), BF16)
        gb = pl.pallas_call(
            start_gather_kernel, in_specs=[vmem] * 2, out_specs=hbm, out_shape=gathered,
            scratch_shapes=[pltpu.VMEM((3, nb, wid), BF16), dma, dma, dma((3, 6))],
            compiler_params=params, name='gather_start')(z, expand(wb_s))
        z1, hbuf = attention(z, gb, wqkvg_s, wo_s, w1, w2, bm, pm, False, heads, bdevs, pdevs, n)
        cols, gb = pl.pallas_call(
            functools.partial(end_gather_kernel, devs, pdevs), in_specs=[hbm, vmem, vmem], out_specs=[vmem, hbm],
            out_shape=[jax.ShapeDtypeStruct((per, n, c), F32), gathered],
            scratch_shapes=[pltpu.VMEM((devs, pad, c), BF16), pltpu.VMEM((3, nb, wid), BF16), dma, dma, dma((3, 6)), dma],
            compiler_params=params, name='gather_end')(hbuf, um, expand(wb_e))
        dbuf, = attention(cols, gb, wqkvg_e, wo_e, w1, w2, bm, pm, True, heads, bdevs, pdevs, n)
        rbuf = all_to_all(dbuf, devs)
        return pl.pallas_call(
            functools.partial(finish_kernel, pdevs), in_specs=[vmem] * 3, out_specs=vmem,
            out_shape=jax.ShapeDtypeStruct(z.shape, F32), compiler_params=pltpu.CompilerParams(vmem_limit_bytes=32 * 2**20), name='finish')(rbuf, um, z1)

    return jax.shard_map(local_fn, mesh=mesh, in_specs=(row_spec,) + (P(),) * 8, out_specs=row_spec, check_vma=False)
```

```python
import functools
import math
import jax
import jax.numpy as jnp
import numpy as np
from jax import lax
from jax.experimental import pallas as pl
from jax.experimental.pallas import tpu as pltpu
from jax.sharding import PartitionSpec as P

F32, BF16 = jnp.float32, jnp.bfloat16
MESH = pl.DeviceIdType.MESH
LOG2E = math.log2(math.e)
EPS = 1e-5
X, Y, Z = 0, 1, 2
DEV = (2, 8, 32)
DIMS = ((X, Y, Z), (Y, Z, X), (Z, X, Y))
SLOT = ((2, 8, 32), (32, 1, 4), (2, 32, 8))
CORE = (1, 16, 1)


def ln(x):
    mu = jnp.mean(x, axis=-1, keepdims=True)
    c = x - mu
    var = jnp.mean(c * c, axis=-1, keepdims=True)
    return (c * lax.rsqrt(var + EPS)).astype(BF16)


def dotf(a, b):
    return jnp.dot(a, b, preferred_element_type=F32)


def dot_nt(a, b):
    return lax.dot_general(a, b, (((1,), (1,)), ((), ())), preferred_element_type=F32)


def mult(v, k):
    return pl.multiple_of(v, k)


def rcopy(src, dst, ssem, rsem, peer):
    return pltpu.make_async_remote_copy(src_ref=src, dst_ref=dst, send_sem=ssem, recv_sem=rsem, device_id={'sp': peer}, device_id_type=MESH)


def bytes_wait(ref, sem):
    pltpu.make_async_copy(ref, ref, sem).wait()


class Place:
    def __init__(self):
        self.me = lax.axis_index('sp')
        self.core = lax.rem(self.me, 2)
        self.at = [lax.rem(self.me // s, 4) for s in DEV]

    def ring(self, dim, t):
        return self.me + (lax.rem(self.at[dim] + t, 4) - self.at[dim]) * DEV[dim]

    def plane(self, c, t):
        return lax.rem(self.at[DIMS[c][2]] + t, 4)

    def slot(self, c, core=None, **over):
        at = [over.get('xyz'[d], self.at[d]) for d in range(3)]
        core = self.core if core is None else core
        return core * CORE[c] + sum(at[d] * SLOT[c][d] for d in range(3))


def slot_of(c, core, at):
    return core * CORE[c] + sum(at[d] * SLOT[c][d] for d in range(3))


def dest_of(c, plane, k):
    if c == 0:
        return plane * 32 + k
    if c == 1:
        return lax.rem(k, 16) * 8 + plane * 2 + k // 16
    return (k // 8) * 32 + plane * 8 + lax.rem(k, 8)


class Gather:
    def __init__(self, place, b_ref, g_ref, ssem, rsem):
        self.p, self.b, self.g, self.ssem, self.rsem = place, b_ref, g_ref, ssem, rsem

    def push(self, c, slot, peer, k):
        rcopy(self.g.at[c, slot], self.g.at[c, slot], self.ssem, self.rsem.at[c, k], peer).start()

    def first(self):
        p = self.p
        for c in range(3):
            slot = slot_of(c, p.core, p.at)
            for t in (1, 3, 2):
                rcopy(self.b.at[c], self.g.at[c, slot], self.ssem, self.rsem.at[c, 0], p.ring(DIMS[c][0], t)).start()
            rcopy(self.b.at[c], self.g.at[c, slot], self.ssem, self.rsem.at[c, 5], p.me ^ 1).start()
        for c in range(3):
            self.g[c, slot_of(c, p.core, p.at)] = self.b[c]

    def second(self):
        p = self.p
        for c in range(3):
            a, b, _ = DIMS[c]
            bytes_wait(self.g.at[c, pl.ds(0, 3)], self.rsem.at[c, 0])

            def body(j, _):
                at = list(p.at)
                at[a] = j
                slot = slot_of(c, p.core, at)
                own = j == p.at[a]

                @pl.when(own)
                def _():
                    for t in (1, 3, 2):
                        rcopy(self.b.at[c], self.g.at[c, slot], self.ssem, self.rsem.at[c, 1], p.ring(b, t)).start()

                @pl.when(jnp.logical_not(own))
                def _():
                    for t in (1, 3, 2):
                        self.push(c, slot, p.ring(b, t), 1)
                    self.push(c, slot, p.me ^ 1, 5)
                return 0
            lax.fori_loop(0, 4, body, 0)

    def third(self):
        p = self.p
        for c in range(3):
            a, b, d = DIMS[c]
            bytes_wait(self.g.at[c, pl.ds(0, 12)], self.rsem.at[c, 1])

            def body(j, _):
                at = list(p.at)
                at[a] = lax.rem(j, 4)
                at[b] = j // 4
                slot = slot_of(c, p.core, at)
                self.push(c, slot, p.ring(d, 1), 2)
                self.push(c, slot, p.ring(d, 3), 3)

                @pl.when(at[b] != p.at[b])
                def _():
                    self.push(c, slot, p.me ^ 1, 5)
                return 0
            lax.fori_loop(0, 16, body, 0)

    def plane_body(self, c, t, fn):
        p = self.p
        a, b, d = DIMS[c]

        def body(j, _):
            at = list(p.at)
            at[a] = lax.rem(j, 4)
            at[b] = j // 4
            at[d] = lax.rem(p.at[d] + t, 4)
            fn(j, slot_of(c, p.core, at))
            return 0
        lax.fori_loop(0, 16, body, 0)

    def forward(self):
        p = self.p
        for side in range(2):
            for c in range(3):
                bytes_wait(self.g.at[c, pl.ds(0, 16)], self.rsem.at[c, 2 + side])
                to = p.ring(DIMS[c][2], 1 if side == 0 else 3)

                def fn(j, slot):
                    @pl.when(j // 8 == side)
                    def _():
                        self.push(c, slot, to, 4)
                    self.push(c, slot, p.me ^ 1, 6 + side)
                self.plane_body(c, 3 if side == 0 else 1, fn)

    def last(self):
        for c in range(3):
            bytes_wait(self.g.at[c, pl.ds(0, 16)], self.rsem.at[c, 4])
            self.plane_body(c, 2, lambda j, slot: self.push(c, slot, self.p.me ^ 1, 8))

    def partner_wait(self, k):
        for c in range(3):
            bytes_wait(self.g.at[c, pl.ds(0, 16)], self.rsem.at[c, k])

    def drain(self):
        for c in range(3):
            bytes_wait(self.g.at[c, pl.ds(0, 127)], self.ssem)


def load_rows(z_ref, xc_ref):
    def body(i, _):
        for r2 in range(2):
            v = z_ref[i, pl.ds(r2, 128, stride=6), :]
            for p in range(4):
                xc_ref[i, pl.ds(p * 64 + r2 * 32, 32), :] = v[p * 32:(p + 1) * 32]
            for x in range(4):
                for core in range(2):
                    xc_ref[i, pl.ds(256 + x * 64 + r2 * 32 + core * 16, 16), :] = z_ref[i, pl.ds((x * 2 + core) * 6 + 2 + r2, 16, stride=48), :]
            for y in range(4):
                for zz in range(4):
                    xc_ref[i, pl.ds(512 + y * 64 + r2 * 32 + zz * 8, 8), :] = z_ref[i, pl.ds((zz * 32 + y * 8) * 6 + 4 + r2, 8, stride=6), :]
        return 0
    lax.fori_loop(0, z_ref.shape[0], body, 0)


def store_rows(place, y_ref, hb_ref, t):
    def body(i, _):
        for r2 in range(2):
            p0, p1, p2 = (place.plane(c, t) for c in range(3))
            y_ref[i, pl.ds(p0 * 192 + r2, 32, stride=6), :] = hb_ref[i, pl.ds(r2 * 32, 32), :]
            for core in range(2):
                y_ref[i, pl.ds(p1 * 12 + core * 6 + 2 + r2, 16, stride=48), :] = hb_ref[i, pl.ds(64 + r2 * 32 + core * 16, 16), :]
            for zz in range(4):
                y_ref[i, pl.ds(p2 * 48 + zz * 192 + 4 + r2, 8, stride=6), :] = hb_ref[i, pl.ds(128 + r2 * 32 + zz * 8, 8), :]
        return 0
    lax.fori_loop(0, y_ref.shape[0], body, 0)


def receive_rows(rb_ref, um_ref, xc_ref):
    for c in range(3):
        def body(g, _):
            zz, y = g // 4, lax.rem(g, 4)
            x = rb_ref[c, pl.ds(mult(g * 8, 8), 8)].reshape(128, 128)
            f = dotf(um_ref[...], x)
            for b in range(2):
                for r in range(6):
                    v = f[(b * 6 + r) * 8:(b * 6 + r + 1) * 8]
                    r2 = r % 2
                    if r // 2 == 0:
                        xc_ref[2 * c + b, pl.ds(mult(zz * 64 + r2 * 32 + y * 8, 8), 8), :] = v
                    elif r // 2 == 2:
                        xc_ref[2 * c + b, pl.ds(mult(512 + y * 64 + r2 * 32 + zz * 8, 8), 8), :] = v
                    else:
                        for core in range(2):
                            xc_ref[2 * c + b, pl.ds(256 + r2 * 32 + core * 16 + g, 4, stride=64), :] = v[core * 4:core * 4 + 4]
            return 0
        lax.fori_loop(0, 16, body, 0)


def finish_rows(rb_ref, um_ref, y_ref):
    for c in range(3):
        def body(g, _):
            x = rb_ref[c, pl.ds(mult(g * 8, 8), 8)].reshape(128, 128)
            f = dotf(um_ref[...], x)
            for b in range(2):
                for r in range(6):
                    at = pl.ds(g * 48 + r, 8, stride=6)
                    y_ref[2 * c + b, at, :] = y_ref[2 * c + b, at, :] + f[(b * 6 + r) * 8:(b * 6 + r + 1) * 8]
            return 0
        lax.fori_loop(0, 16, body, 0)


def stage(end, place, gather, heads, xc_ref, b_ref, gb_ref, w_ref, wb_ref, wo_ref, w1_ref, w2_ref, bm_ref, pm_ref, y_ref, rb_ref, esem, fsem,
          u_ref, q_ref, g_ref, kT_ref, v_ref, bf_ref, hb_ref, sb_ref):
    per, n, c = xc_ref.shape
    hd = c // heads
    nq = n // 4
    scale = hd ** -0.5 * LOG2E
    me = place.me

    for col in range(3):
        acc = None
        for r2 in range(2):
            i = col * 2 + r2
            u = ln(xc_ref[i])
            u_ref[i] = u
            t = dot_nt(wb_ref[r2], u)
            acc = t if acc is None else acc + t
        b_ref[col] = acc.astype(BF16)
    gather.first()

    wkT = w_ref[:, c:2 * c].T

    def project(i, _):
        u = u_ref[i]
        kT_ref[i] = dot_nt(wkT, u).astype(BF16)
        q_ref[i] = dotf(u, w_ref[:, :c]).astype(BF16)
        vg = dotf(u, w_ref[:, 2 * c:])
        v_ref[i, :, :c] = vg[:, :c].astype(BF16)
        v_ref[i, :, c:] = jnp.ones((n, c), BF16)
        g_ref[i] = jax.nn.sigmoid(vg[:, c:])
        return 0

    lax.fori_loop(0, per // 2, project, 0)
    gather.second()
    lax.fori_loop(per // 2, per, project, 0)
    gather.third()

    def block(step, _):
        t = jnp.where(step == 1, 3, jnp.where(step == 2, 1, jnp.where(step == 3, 2, 0)))
        for k, sem in ((0, 5), (1, 6), (2, 7), (3, 8)):
            @pl.when(step == k)
            def _():
                gather.partner_wait(sem)
        planes = [place.plane(col, t) for col in range(3)]
        for col in range(3):
            b = gb_ref[col, pl.ds(mult(planes[col] * 32, 32), 32)].reshape(256, n)
            f = dotf(bm_ref[...], b) * LOG2E
            for h in range(heads):
                bf_ref[h, col * 64:(col + 1) * 64, :] = f[h * 64:(h + 1) * 64]
        rows = [pl.ds(mult(col * 256 + planes[col] * 64, 64), 64) for col in range(3)]

        def row(i, _):
            @pl.when(jnp.logical_and(step == 0, i == 3))
            def _():
                gather.forward()

            @pl.when(jnp.logical_and(step == 1, i == 3))
            def _():
                gather.last()
            qb = jnp.concatenate([q_ref[i, r, :] for r in rows], axis=0)
            lane = lax.broadcasted_iota(jnp.int32, (nq, c), 1) // hd
            res = jnp.zeros((nq, c), F32)
            for h in range(heads):
                qm = jnp.where(lane == h, qb, jnp.zeros_like(qb))
                s = dotf(qm, kT_ref[i])
                s = s * scale + bf_ref[h]
                m = jnp.max(s, axis=-1, keepdims=True)
                p = jnp.exp2(s - m).astype(BF16)
                o = dotf(p, v_ref[i])
                res = jnp.where(lane == h, o[:, :c] / o[:, c:], res)
            og = (res * jnp.concatenate([g_ref[i, r, :] for r in rows], axis=0)).astype(BF16)
            upd = dotf(og, wo_ref[...])
            if end:
                hb_ref[i] = upd
            else:
                hb_ref[i] = jnp.concatenate([xc_ref[i, r, :] for r in rows], axis=0) + upd
            return 0
        lax.fori_loop(0, per, row, 0)

        if end:
            def trans(i, _):
                upd = jnp.concatenate([hb_ref[2 * i], hb_ref[2 * i + 1]], axis=0)
                two = jnp.concatenate([xc_ref[2 * i + a, r, :] for a in range(2) for r in rows], axis=0) + upd
                hid = jnp.maximum(dotf(ln(two), w1_ref[...]), 0).astype(BF16)
                new = upd + dotf(hid, w2_ref[...])
                hb_ref[2 * i] = new[:nq]
                hb_ref[2 * i + 1] = new[nq:]
                return 0
            lax.fori_loop(0, per // 2, trans, 0)
        else:
            store_rows(place, y_ref, hb_ref, t)

        def pack(kg, _):
            for col in range(3):
                x = jnp.concatenate([hb_ref[i, pl.ds(mult(col * 64 + r2 * 32 + kg * 8, 8), 8), :] for i in range(per) for r2 in range(2)], axis=0)
                f = dotf(pm_ref[...], x.astype(BF16)).reshape(8, 16, c).astype(BF16)
                sb_ref[col, pl.ds(mult(planes[col] * 32 + kg * 8, 8), 8)] = f
            return 0
        lax.fori_loop(0, 4, pack, 0)

        def send(k, _):
            for col in range(3):
                slot = planes[col] * 32 + k
                d = dest_of(col, planes[col], k)

                @pl.when(d != me)
                def _():
                    rcopy(sb_ref.at[col, slot], rb_ref.at[col, me], fsem, esem, d).start()
            return 0
        lax.fori_loop(0, 32, send, 0)
        return 0
    lax.fori_loop(0, 4, block, 0)
    for col in range(3):
        rb_ref[col, me] = sb_ref[col, slot_of(col, place.core, place.at)]
    gather.drain()
    bytes_wait(rb_ref.at[:, pl.ds(0, 127)], fsem)
    bytes_wait(rb_ref.at[:, pl.ds(0, 127)], esem)


def kernel(heads, z_ref, ws_ref, wos_ref, we_ref, woe_ref, w1_ref, w2_ref, wb_ref, bm_ref, pm_ref, um1_ref, um2_ref, y_ref,
           xc_ref, b_ref, gb1_ref, gb2_ref, rb1_ref, rb2_ref, u_ref, q_ref, g_ref, kT_ref, v_ref, bf_ref, hb_ref, sb_ref,
           gs1, gr1, gs2, gr2, e1, f1, e2, f2):
    place = Place()
    work = (u_ref, q_ref, g_ref, kT_ref, v_ref, bf_ref, hb_ref, sb_ref)
    load_rows(z_ref, xc_ref)
    stage(False, place, Gather(place, b_ref.at[0], gb1_ref, gs1, gr1), heads, xc_ref, b_ref.at[0], gb1_ref, ws_ref, wb_ref.at[0], wos_ref, w1_ref, w2_ref,
          bm_ref, pm_ref, y_ref, rb1_ref, e1, f1, *work)
    receive_rows(rb1_ref, um1_ref, xc_ref)
    stage(True, place, Gather(place, b_ref.at[1], gb2_ref, gs2, gr2), heads, xc_ref, b_ref.at[1], gb2_ref, we_ref, wb_ref.at[1], woe_ref, w1_ref, w2_ref,
          bm_ref, pm_ref, y_ref, rb2_ref, e2, f2, *work)
    finish_rows(rb2_ref, um2_ref, y_ref)


def pack_matrix():
    m = np.zeros((8, 16, 6, 2, 8), np.float32)
    for k in range(8):
        for i in range(6):
            for r in range(2):
                m[k, i * 2 + r, i, r, k] = 1
    return jnp.asarray(m.reshape(128, 96), BF16)


def unpack_matrix(swap):
    m = np.zeros((2, 6, 8, 8, 16), np.float32)
    for k in range(8):
        for i in range(6):
            for r in range(2):
                row = (k % 2) * 4 + k // 2 if swap and i // 2 == 1 else k
                m[r, i, row, k, i * 2 + r] = 1
    return jnp.asarray(m.reshape(96, 128), BF16)


def bias_matrix(heads):
    m = np.zeros((heads, 2, 32, 32, 2, heads), np.float32)
    for k in range(32):
        for r in range(2):
            for h in range(heads):
                m[h, r, k, k, r, h] = 1
    return jnp.asarray(m.reshape(256, 256), BF16)


def solution(mesh):
    devs = mesh.shape['sp']
    row_spec = P(('dp', 'sp'), None, None)
    vmem = pl.BlockSpec(memory_space=pltpu.VMEM)
    dma = pltpu.SemaphoreType.DMA

    def local_fn(z, wqkvg_s, wb_s, wo_s, wqkvg_e, wb_e, wo_e, w1, w2):
        per, n, c = z.shape
        heads = wb_s.shape[0]
        wb = jnp.stack([wb_s, wb_e])
        none = jnp.zeros_like(wb)
        wb = jnp.stack([jnp.concatenate([wb, none], 1), jnp.concatenate([none, wb], 1)], 1)
        args = (z, wqkvg_s, wo_s, wqkvg_e, wo_e, w1, w2, wb, bias_matrix(heads), pack_matrix(), unpack_matrix(True), unpack_matrix(False))
        return pl.pallas_call(
            functools.partial(kernel, heads), in_specs=[vmem] * len(args), out_specs=vmem,
            out_shape=jax.ShapeDtypeStruct(z.shape, F32),
            scratch_shapes=[
                pltpu.VMEM((per, n, c), F32), pltpu.VMEM((2, 3, 8, n), BF16),
                pltpu.VMEM((3, devs, 8, n), BF16), pltpu.VMEM((3, devs, 8, n), BF16),
                pltpu.VMEM((3, devs, 16, c), BF16), pltpu.VMEM((3, devs, 16, c), BF16),
                pltpu.VMEM((per, n, c), BF16), pltpu.VMEM((per, n, c), BF16), pltpu.VMEM((per, n, c), F32),
                pltpu.VMEM((per, c, n), BF16), pltpu.VMEM((per, n, 2 * c), BF16), pltpu.VMEM((heads, n // 4, n), F32),
                pltpu.VMEM((per, n // 4, c), F32), pltpu.VMEM((3, devs, 16, c), BF16),
                dma, dma((3, 9)), dma, dma((3, 9)), dma, dma, dma, dma],
            compiler_params=pltpu.CompilerParams(has_side_effects=True, vmem_limit_bytes=60 * 2**20), name='block')(*args)

    return jax.shard_map(local_fn, mesh=mesh, in_specs=(row_spec,) + (P(),) * 8, out_specs=row_spec, check_vma=False)
```

```python
import functools
import math
import jax
import jax.numpy as jnp
import numpy as np
from jax import lax
from jax.experimental import pallas as pl
from jax.experimental.pallas import tpu as pltpu
from jax.sharding import PartitionSpec as P

F32, BF16 = jnp.float32, jnp.bfloat16
MESH = pl.DeviceIdType.MESH
LOG2E = math.log2(math.e)
EPS = 1e-5
X, Y, Z = 0, 1, 2
DEV = (2, 8, 32)
DIMS = ((X, Y, Z), (Y, Z, X), (Z, X, Y))
SLOT = ((1, 4, 32), (32, 1, 4), (4, 32, 1))


def ln(x):
    mu = jnp.mean(x, axis=-1, keepdims=True)
    c = x - mu
    var = jnp.mean(c * c, axis=-1, keepdims=True)
    return (c * lax.rsqrt(var + EPS)).astype(BF16)


def dotf(a, b):
    return jnp.dot(a, b, preferred_element_type=F32)


def dot_nt(a, b):
    return lax.dot_general(a, b, (((1,), (1,)), ((), ())), preferred_element_type=F32)


def mult(v, k):
    return pl.multiple_of(v, k)


def rcopy(src, dst, ssem, rsem, peer):
    return pltpu.make_async_remote_copy(src_ref=src, dst_ref=dst, send_sem=ssem, recv_sem=rsem, device_id={'sp': peer}, device_id_type=MESH)


def bytes_wait(ref, sem):
    pltpu.make_async_copy(ref, ref, sem).wait()


class Place:
    def __init__(self):
        self.me = lax.axis_index('sp')
        self.core = lax.rem(self.me, 2)
        self.at = [lax.rem(self.me // s, 4) for s in DEV]

    def ring(self, dim, t):
        return self.me + (lax.rem(self.at[dim] + t, 4) - self.at[dim]) * DEV[dim]

    def plane(self, c, t):
        return lax.rem(self.at[DIMS[c][2]] + t, 4)


def slot_of(c, place):
    return place.core * 16 + sum(place.at[d] * SLOT[c][d] for d in range(3))


def dest_of(c, plane, k):
    if c == 0:
        return plane * 32 + lax.rem(k, 16) * 2 + k // 16
    if c == 1:
        return lax.rem(k, 16) * 8 + plane * 2 + k // 16
    return lax.rem(k, 4) * 32 + plane * 8 + lax.rem(k // 4, 4) * 2 + k // 16


class Gather:
    def __init__(self, place, b_ref, g_ref, ssem, rsem):
        self.p, self.b, self.g, self.ssem, self.rsem = place, b_ref, g_ref, ssem, rsem

    def push(self, c, start, count, peer, k):
        part = self.g.at[c, pl.ds(start, count)]
        rcopy(part, part, self.ssem, self.rsem.at[c, k], peer).start()

    def half(self, c, t):
        return self.p.plane(c, t) * 32 + self.p.core * 16

    def first(self):
        p = self.p
        for c in range(3):
            slot = slot_of(c, p)
            for t in (1, 3, 2):
                rcopy(self.b.at[c], self.g.at[c, slot], self.ssem, self.rsem.at[c, 0], p.ring(DIMS[c][0], t)).start()
        for c in range(3):
            self.g[c, slot_of(c, p)] = self.b[c]

    def second(self):
        p = self.p
        for c in range(3):
            b = DIMS[c][1]
            bytes_wait(self.g.at[c, pl.ds(0, 3)], self.rsem.at[c, 0])
            for t in (1, 3, 2):
                self.push(c, self.half(c, 0) + p.at[b] * 4, 4, p.ring(b, t), 1)

    def third(self):
        p = self.p
        for c in range(3):
            d = DIMS[c][2]
            bytes_wait(self.g.at[c, pl.ds(0, 12)], self.rsem.at[c, 1])
            self.push(c, self.half(c, 0), 16, p.me ^ 1, 5)
            self.push(c, self.half(c, 0), 16, p.ring(d, 1), 2)
            self.push(c, self.half(c, 0), 16, p.ring(d, 3), 3)

    def forward(self):
        p = self.p
        for side, t in ((0, 3), (1, 1)):
            for c in range(3):
                bytes_wait(self.g.at[c, pl.ds(0, 16)], self.rsem.at[c, 2 + side])
                self.push(c, self.half(c, t), 16, p.me ^ 1, 6 + side)
                self.push(c, self.half(c, t) + side * 8, 8, p.ring(DIMS[c][2], 4 - t), 4)

    def last(self):
        for c in range(3):
            bytes_wait(self.g.at[c, pl.ds(0, 16)], self.rsem.at[c, 4])
            self.push(c, self.half(c, 2), 16, self.p.me ^ 1, 8)

    def partner_wait(self, k):
        for c in range(3):
            bytes_wait(self.g.at[c, pl.ds(0, 16)], self.rsem.at[c, k])

    def drain(self):
        for c in range(3):
            bytes_wait(self.g.at[c, pl.ds(0, 127)], self.ssem)


def load_rows(z_ref, xc_ref):
    def body(i, _):
        for r2 in range(2):
            for p in range(4):
                for core in range(2):
                    at = p * 64 + r2 * 32 + core * 16
                    xc_ref[i, pl.ds(at, 16), :] = z_ref[i, pl.ds((p * 32 + core) * 6 + r2, 16, stride=12), :]
                    xc_ref[i, pl.ds(256 + at, 16), :] = z_ref[i, pl.ds((p * 2 + core) * 6 + 2 + r2, 16, stride=48), :]
                    for x in range(4):
                        xc_ref[i, pl.ds(512 + at + x * 4, 4), :] = z_ref[i, pl.ds((p * 8 + x * 2 + core) * 6 + 4 + r2, 4, stride=192), :]
        return 0
    lax.fori_loop(0, z_ref.shape[0], body, 0)


def store_rows(place, y_ref, hb_ref, t):
    def body(i, _):
        p0, p1, p2 = (place.plane(c, t) for c in range(3))
        for r2 in range(2):
            for core in range(2):
                at = r2 * 32 + core * 16
                y_ref[i, pl.ds(p0 * 192 + core * 6 + r2, 16, stride=12), :] = hb_ref[i, pl.ds(at, 16), :]
                y_ref[i, pl.ds(p1 * 12 + core * 6 + 2 + r2, 16, stride=48), :] = hb_ref[i, pl.ds(64 + at, 16), :]
                for x in range(4):
                    y_ref[i, pl.ds(p2 * 48 + x * 12 + core * 6 + 4 + r2, 4, stride=192), :] = hb_ref[i, pl.ds(128 + at + x * 4, 4), :]
        return 0
    lax.fori_loop(0, y_ref.shape[0], body, 0)


def receive_rows(rb_ref, um_ref, xc_ref):
    for c in range(3):
        def body(zz, _):
            for y in range(4):
                x = rb_ref[c, pl.ds(mult(zz * 32 + y * 8, 8), 8)].reshape(128, 128)
                f = dotf(um_ref[...], x)
                for b in range(2):
                    for r in range(6):
                        for core in range(2):
                            v = f[(b * 6 + r) * 8 + core * 4:(b * 6 + r) * 8 + core * 4 + 4]
                            at = (r % 2) * 32 + core * 16
                            if r // 2 == 0:
                                xc_ref[2 * c + b, pl.ds(mult(zz * 64, 64) + at + y * 4, 4), :] = v
                            elif r // 2 == 1:
                                xc_ref[2 * c + b, pl.ds(256 + at + zz * 4 + y, 4, stride=64), :] = v
                            else:
                                xc_ref[2 * c + b, pl.ds(512 + at + y * 64 + zz, 4, stride=4), :] = v
            return 0
        lax.fori_loop(0, 4, body, 0)


def finish_rows(rb_ref, um_ref, y_ref):
    for c in range(3):
        def body(g, _):
            x = rb_ref[c, pl.ds(mult(g * 8, 8), 8)].reshape(128, 128)
            f = dotf(um_ref[...], x)
            for b in range(2):
                for r in range(6):
                    at = pl.ds(g * 48 + r, 8, stride=6)
                    y_ref[2 * c + b, at, :] = y_ref[2 * c + b, at, :] + f[(b * 6 + r) * 8:(b * 6 + r + 1) * 8]
            return 0
        lax.fori_loop(0, 16, body, 0, unroll=4)


def stage(end, place, gather, heads, xc_ref, b_ref, gb_ref, w_ref, wb_ref, wo_ref, w1_ref, w2_ref, bm_ref, pm_ref, y_ref, rb_ref, esem, fsem,
          u_ref, q_ref, g_ref, kT_ref, v_ref, bf_ref, hb_ref, sb_ref, s_refs, p_refs):
    per, n, c = xc_ref.shape
    hd = c // heads
    nq = n // 4
    scale = hd ** -0.5 * LOG2E
    me = place.me

    for col in range(3):
        acc = None
        for r2 in range(2):
            i = col * 2 + r2
            u = ln(xc_ref[i])
            u_ref[i] = u
            t = dot_nt(wb_ref[r2], u)
            acc = t if acc is None else acc + t
        b_ref[col] = acc.astype(BF16)
    gather.first()

    wkT = w_ref[:, c:2 * c].T

    def project(i, _):
        u = u_ref[i]
        kT_ref[i] = dot_nt(wkT, u).astype(BF16)
        q_ref[i] = dotf(u, w_ref[:, :c]).astype(BF16)
        vg = dotf(u, w_ref[:, 2 * c:])
        v_ref[i, :, :c] = vg[:, :c].astype(BF16)
        v_ref[i, :, c:] = jnp.ones((n, c), BF16)
        g_ref[i] = jax.nn.sigmoid(vg[:, c:])
        return 0

    lax.fori_loop(0, per // 2, project, 0)
    gather.second()
    lax.fori_loop(per // 2, per, project, 0)
    gather.third()

    order = (0, 3, 1, 2)

    def pick(step):
        return jnp.where(step == 1, 3, jnp.where(step == 2, 1, jnp.where(step == 3, 2, 0)))

    def send(col, plane, o):
        k = lax.rem(slot_of(col, place), 32) ^ o
        rcopy(sb_ref.at[col, plane * 32 + k], rb_ref.at[col, me], fsem, esem, dest_of(col, plane, k)).start()

    def block(step, _):
        first = isinstance(step, int)
        t = 0 if first else pick(step)
        before = None if first else [place.plane(col, pick(step - 1)) for col in range(3)]
        gather.partner_wait(5 + step)
        planes = [place.plane(col, t) for col in range(3)]
        for col in range(3):
            b = gb_ref[col, pl.ds(mult(planes[col] * 32, 32), 32)].reshape(256, n)
            f = dotf(bm_ref[...], b) * LOG2E
            for h in range(heads):
                bf_ref[h * nq + col * 64:h * nq + (col + 1) * 64, :] = f[h * 64:(h + 1) * 64]
        rows = [pl.ds(mult(col * 256 + planes[col] * 64, 64), 64) for col in range(3)]

        lane = lax.broadcasted_iota(jnp.int32, (nq, c), 1) // hd

        def scores(i):
            qb = jnp.concatenate([q_ref[i, r, :] for r in rows], axis=0)
            qm = jnp.concatenate([jnp.where(lane == h, qb, jnp.zeros_like(qb)) for h in range(heads)], axis=0)
            s_refs[i % 2][...] = dotf(qm, kT_ref[i]) * scale + bf_ref[...]

        def soften(i):
            t = s_refs[i % 2][...]
            m = jnp.max(t, axis=-1, keepdims=True)
            p_refs[i % 2][...] = jnp.exp2(t - m).astype(BF16)

        def mix(i):
            o = dotf(p_refs[i % 2][...], v_ref[i])
            o = o[:, :c] / o[:, c:]
            res = jnp.zeros((nq, c), F32)
            for h in range(heads):
                res = jnp.where(lane == h, o[h * nq:(h + 1) * nq], res)
            og = (res * jnp.concatenate([g_ref[i, r, :] for r in rows], axis=0)).astype(BF16)
            upd = dotf(og, wo_ref[...])
            if end:
                hb_ref[i] = upd
            else:
                hb_ref[i] = jnp.concatenate([xc_ref[i, r, :] for r in rows], axis=0) + upd

        if not first:
            @pl.when(step > 1)
            def _():
                for col in range(3):
                    send(col, before[col], 0)
        scores(0)
        for i in range(per):
            if not first:
                for o in range(1 + i * 31 // per, 1 + (i + 1) * 31 // per):
                    for col in range(3):
                        send(col, before[col], o)
            if i + 1 < per:
                scores(i + 1)
            soften(i)
            if i > 0:
                mix(i - 1)
        mix(per - 1)
        if first:
            gather.forward()
        else:
            @pl.when(step == 1)
            def _():
                gather.last()

        if end:
            def trans(i, _):
                upd = jnp.concatenate([hb_ref[2 * i], hb_ref[2 * i + 1]], axis=0)
                two = jnp.concatenate([xc_ref[2 * i + a, r, :] for a in range(2) for r in rows], axis=0) + upd
                hid = jnp.maximum(dotf(ln(two), w1_ref[...]), 0).astype(BF16)
                new = upd + dotf(hid, w2_ref[...])
                hb_ref[2 * i] = new[:nq]
                hb_ref[2 * i + 1] = new[nq:]
                return 0
            lax.fori_loop(0, per // 2, trans, 0, unroll=3)
        else:
            store_rows(place, y_ref, hb_ref, t)

        def pack(kg, _):
            for col in range(3):
                x = jnp.concatenate([hb_ref[i, pl.ds(mult(col * 64 + r2 * 32 + kg * 8, 8), 8), :] for i in range(per) for r2 in range(2)], axis=0)
                f = dotf(pm_ref[...], x.astype(BF16)).reshape(8, 16, c).astype(BF16)
                sb_ref[col, pl.ds(mult(planes[col] * 32 + kg * 8, 8), 8)] = f
            return 0
        lax.fori_loop(0, 4, pack, 0, unroll=4)

        return 0

    block(0, 0)
    lax.fori_loop(1, 4, block, 0)
    tail = [place.plane(col, order[3]) for col in range(3)]

    def send_tail(o, _):
        for col in range(3):
            send(col, tail[col], o)
        return 0
    lax.fori_loop(0, 32, send_tail, 0)
    for col in range(3):
        rb_ref[col, me] = sb_ref[col, slot_of(col, place)]
    gather.drain()
    bytes_wait(rb_ref.at[:, pl.ds(0, 127)], fsem)
    bytes_wait(rb_ref.at[:, pl.ds(0, 127)], esem)


def kernel(heads, z_ref, ws_ref, wos_ref, we_ref, woe_ref, w1_ref, w2_ref, wb_ref, bm_ref, pm_ref, um1_ref, um2_ref, y_ref,
           xc_ref, b_ref, gb1_ref, gb2_ref, rb1_ref, rb2_ref, u_ref, q_ref, g_ref, kT_ref, v_ref, bf_ref, hb_ref, sb_ref, sa_ref, sb2_ref, pa_ref, pb_ref,
           gs1, gr1, gs2, gr2, e1, f1, e2, f2):
    place = Place()
    work = (u_ref, q_ref, g_ref, kT_ref, v_ref, bf_ref, hb_ref, sb_ref, (sa_ref, sb2_ref), (pa_ref, pb_ref))
    load_rows(z_ref, xc_ref)
    stage(False, place, Gather(place, b_ref.at[0], gb1_ref, gs1, gr1), heads, xc_ref, b_ref.at[0], gb1_ref, ws_ref, wb_ref.at[0], wos_ref, w1_ref, w2_ref,
          bm_ref, pm_ref, y_ref, rb1_ref, e1, f1, *work)
    receive_rows(rb1_ref, um1_ref, xc_ref)
    stage(True, place, Gather(place, b_ref.at[1], gb2_ref, gs2, gr2), heads, xc_ref, b_ref.at[1], gb2_ref, we_ref, wb_ref.at[1], woe_ref, w1_ref, w2_ref,
          bm_ref, pm_ref, y_ref, rb2_ref, e2, f2, *work)
    finish_rows(rb2_ref, um2_ref, y_ref)


def pack_matrix():
    m = np.zeros((8, 16, 6, 2, 8), np.float32)
    for k in range(8):
        for i in range(6):
            for r in range(2):
                m[k, i * 2 + r, i, r, k] = 1
    return jnp.asarray(m.reshape(128, 96), BF16)


def unpack_matrix(swap):
    m = np.zeros((2, 6, 8, 8, 16), np.float32)
    for k in range(8):
        for i in range(6):
            for r in range(2):
                row = (k % 2) * 4 + k // 2 if swap else k
                m[r, i, row, k, i * 2 + r] = 1
    return jnp.asarray(m.reshape(96, 128), BF16)


def bias_matrix(heads):
    m = np.zeros((heads, 2, 32, 32, 2, heads), np.float32)
    for k in range(32):
        for r in range(2):
            for h in range(heads):
                m[h, r, k, k, r, h] = 1
    return jnp.asarray(m.reshape(256, 256), BF16)


def solution(mesh):
    devs = mesh.shape['sp']
    row_spec = P(('dp', 'sp'), None, None)
    vmem = pl.BlockSpec(memory_space=pltpu.VMEM)
    dma = pltpu.SemaphoreType.DMA

    def local_fn(z, wqkvg_s, wb_s, wo_s, wqkvg_e, wb_e, wo_e, w1, w2):
        per, n, c = z.shape
        heads = wb_s.shape[0]
        wb = jnp.stack([wb_s, wb_e])
        none = jnp.zeros_like(wb)
        wb = jnp.stack([jnp.concatenate([wb, none], 1), jnp.concatenate([none, wb], 1)], 1)
        args = (z, wqkvg_s, wo_s, wqkvg_e, wo_e, w1, w2, wb, bias_matrix(heads), pack_matrix(), unpack_matrix(True), unpack_matrix(False))
        return pl.pallas_call(
            functools.partial(kernel, heads), in_specs=[vmem] * len(args), out_specs=vmem,
            out_shape=jax.ShapeDtypeStruct(z.shape, F32),
            scratch_shapes=[
                pltpu.VMEM((per, n, c), F32), pltpu.VMEM((2, 3, 8, n), BF16),
                pltpu.VMEM((3, devs, 8, n), BF16), pltpu.VMEM((3, devs, 8, n), BF16),
                pltpu.VMEM((3, devs, 16, c), BF16), pltpu.VMEM((3, devs, 16, c), BF16),
                pltpu.VMEM((per, n, c), BF16), pltpu.VMEM((per, n, c), BF16), pltpu.VMEM((per, n, c), F32),
                pltpu.VMEM((per, c, n), BF16), pltpu.VMEM((per, n, 2 * c), BF16), pltpu.VMEM((heads * n // 4, n), F32),
                pltpu.VMEM((per, n // 4, c), F32), pltpu.VMEM((3, devs, 16, c), BF16),
                pltpu.VMEM((heads * n // 4, n), F32), pltpu.VMEM((heads * n // 4, n), F32),
                pltpu.VMEM((heads * n // 4, n), BF16), pltpu.VMEM((heads * n // 4, n), BF16),
                dma, dma((3, 9)), dma, dma((3, 9)), dma, dma, dma, dma],
            compiler_params=pltpu.CompilerParams(has_side_effects=True, vmem_limit_bytes=60 * 2**20), name='block')(*args)

    return jax.shard_map(local_fn, mesh=mesh, in_specs=(row_spec,) + (P(),) * 8, out_specs=row_spec, check_vma=False)
```

```python
import functools
import math
import jax
import jax.numpy as jnp
import numpy as np
from jax import lax
from jax.experimental import pallas as pl
from jax.experimental.pallas import tpu as pltpu
from jax.sharding import PartitionSpec as P

F32, BF16 = jnp.float32, jnp.bfloat16
MESH = pl.DeviceIdType.MESH
LOG2E = math.log2(math.e)
EPS = 1e-5
X, Y, Z = 0, 1, 2
COLOURS = range(3)
PAIR = range(2)
QUAD = range(4)
HALF, SIDE, PLANE = 16, 32, 64
DEV = (2, 8, 32)
DIMS = ((X, Y, Z), (Y, Z, X), (Z, X, Y))
SLOT = ((1, 4, 32), (32, 1, 4), (4, 32, 1))


def ln(x):
    mu = jnp.mean(x, axis=-1, keepdims=True)
    c = x - mu
    var = jnp.mean(c * c, axis=-1, keepdims=True)
    return (c * lax.rsqrt(var + EPS)).astype(BF16)


def dotf(a, b):
    return jnp.dot(a, b, preferred_element_type=F32)


def dot_nt(a, b):
    return lax.dot_general(a, b, (((1,), (1,)), ((), ())), preferred_element_type=F32)


def mult(v, k):
    return pl.multiple_of(v, k)


def rcopy(src, dst, ssem, rsem, peer):
    return pltpu.make_async_remote_copy(src_ref=src, dst_ref=dst, send_sem=ssem, recv_sem=rsem, device_id={'sp': peer}, device_id_type=MESH)


def bytes_wait(ref, sem):
    pltpu.make_async_copy(ref, ref, sem).wait()


class Place:
    def __init__(self):
        self.me = lax.axis_index('sp')
        self.core = lax.rem(self.me, 2)
        self.at = [lax.rem(self.me // s, 4) for s in DEV]

    def ring(self, dim, t):
        return self.me + (lax.rem(self.at[dim] + t, 4) - self.at[dim]) * DEV[dim]

    def plane(self, c, t):
        return lax.rem(self.at[DIMS[c][2]] + t, 4)


def slot_of(c, place):
    return place.core * HALF + sum(place.at[d] * SLOT[c][d] for d in COLOURS)


def dest_of(c, plane, k):
    if c == 0:
        return plane * SIDE + lax.rem(k, HALF) * 2 + k // HALF
    if c == 1:
        return lax.rem(k, HALF) * 8 + plane * 2 + k // HALF
    return lax.rem(k, 4) * SIDE + plane * 8 + lax.rem(k // 4, 4) * 2 + k // HALF


class Gather:
    def __init__(self, place, b_ref, g_ref, ssem, rsem):
        self.p, self.b, self.g, self.ssem, self.rsem = place, b_ref, g_ref, ssem, rsem

    def push(self, c, start, count, peer, k):
        part = self.g.at[c, pl.ds(start, count)]
        rcopy(part, part, self.ssem, self.rsem.at[c, k], peer).start()

    def half(self, c, t):
        return self.p.plane(c, t) * SIDE + self.p.core * HALF

    def first(self, c):
        p = self.p
        slot = slot_of(c, p)
        for t in (1, 3, 2):
            rcopy(self.b.at[c], self.g.at[c, slot], self.ssem, self.rsem.at[c, 0], p.ring(DIMS[c][0], t)).start()
        self.g[c, slot] = self.b[c]

    def second(self, c):
        p = self.p
        b = DIMS[c][1]
        bytes_wait(self.g.at[c, pl.ds(0, 3)], self.rsem.at[c, 0])
        for t in (1, 3, 2):
            self.push(c, self.half(c, 0) + p.at[b] * 4, 4, p.ring(b, t), 1)

    def third(self, c):
        p = self.p
        d = DIMS[c][2]
        bytes_wait(self.g.at[c, pl.ds(0, 12)], self.rsem.at[c, 1])
        self.push(c, self.half(c, 0), HALF, p.me ^ 1, 5)
        self.push(c, self.half(c, 0), HALF, p.ring(d, 1), 2)
        self.push(c, self.half(c, 0), HALF, p.ring(d, 3), 3)

    def forward(self):
        p = self.p
        for side, t in ((0, 3), (1, 1)):
            for c in COLOURS:
                bytes_wait(self.g.at[c, pl.ds(0, HALF)], self.rsem.at[c, 2 + side])
                self.push(c, self.half(c, t), HALF, p.me ^ 1, 6 + side)
                self.push(c, self.half(c, t) + side * 8, 8, p.ring(DIMS[c][2], 4 - t), 4)

    def last(self):
        for c in COLOURS:
            bytes_wait(self.g.at[c, pl.ds(0, HALF)], self.rsem.at[c, 4])
            self.push(c, self.half(c, 2), HALF, self.p.me ^ 1, 8)

    def partner_wait(self, k):
        for c in COLOURS:
            bytes_wait(self.g.at[c, pl.ds(0, HALF)], self.rsem.at[c, k])

    def drain(self):
        for c in COLOURS:
            bytes_wait(self.g.at[c, pl.ds(0, 127)], self.ssem)


def load_rows(z_ref, xc_ref):
    def body(i, _):
        for r2 in PAIR:
            for p in QUAD:
                for core in PAIR:
                    at = p * PLANE + r2 * SIDE + core * HALF
                    xc_ref[i, pl.ds(at, HALF), :] = z_ref[i, pl.ds((p * SIDE + core) * 6 + r2, HALF, stride=12), :]
                    xc_ref[i, pl.ds(256 + at, HALF), :] = z_ref[i, pl.ds((p * 2 + core) * 6 + 2 + r2, HALF, stride=48), :]
                    for x in QUAD:
                        xc_ref[i, pl.ds(512 + at + x * 4, 4), :] = z_ref[i, pl.ds((p * 8 + x * 2 + core) * 6 + 4 + r2, 4, stride=192), :]
        return 0
    lax.fori_loop(0, z_ref.shape[0], body, 0)


def store_rows(place, y_ref, hb_ref, t):
    def body(i, _):
        p0, p1, p2 = (place.plane(c, t) for c in COLOURS)
        for r2 in PAIR:
            for core in PAIR:
                at = r2 * SIDE + core * HALF
                y_ref[i, pl.ds(p0 * 192 + core * 6 + r2, HALF, stride=12), :] = hb_ref[i, pl.ds(at, HALF), :]
                y_ref[i, pl.ds(p1 * 12 + core * 6 + 2 + r2, HALF, stride=48), :] = hb_ref[i, pl.ds(PLANE + at, HALF), :]
                for x in QUAD:
                    y_ref[i, pl.ds(p2 * 48 + x * 12 + core * 6 + 4 + r2, 4, stride=192), :] = hb_ref[i, pl.ds(128 + at + x * 4, 4), :]
        return 0
    lax.fori_loop(0, y_ref.shape[0], body, 0)


def inbox(c, place):
    x, y, z = place.at
    if c == 0:
        return place.me
    if c == 1:
        return x * SIDE + z * 8 + y * 2 + place.core
    return y * SIDE + z * 8 + x * 2 + place.core


def each_plane(place, rb_ref, esem, fn):
    def body(step, _):
        @pl.when(step == 0)
        def _():
            bytes_wait(rb_ref.at[:, pl.ds(0, 31)], esem.at[step])

        @pl.when(step > 0)
        def _():
            bytes_wait(rb_ref.at[:, pl.ds(0, SIDE)], esem.at[step])
        t = jnp.where(step == 1, 1, jnp.where(step == 2, 3, jnp.where(step == 3, 2, 0)))
        for c in COLOURS:
            q = place.plane(c, t)
            for g in QUAD:
                fn(c, q, g, rb_ref[c, pl.ds(mult(q * SIDE + g * 8, 8), 8)].reshape(96, 128))
        return 0
    lax.fori_loop(0, 4, body, 0)


def receive_rows(place, rb_ref, esem, um_ref, xc_ref):
    def put(c, q, g, x):
        f = dotf(um_ref[...], x)
        for b in PAIR:
            for r in range(6):
                for core in PAIR:
                    v = f[(b * 6 + r) * 8 + core * 4:(b * 6 + r) * 8 + core * 4 + 4]
                    at = (r % 2) * SIDE + core * HALF
                    if c == 1:
                        rows = (pl.ds(g * PLANE + at + q, 4, stride=4), pl.ds(mult(q * PLANE, PLANE) + 256 + at + g * 4, 4), pl.ds(512 + at + q * 4 + g, 4, stride=PLANE))
                    else:
                        zz, y = (q, g) if c == 0 else (g, q)
                        first = pl.ds(mult(q * PLANE, PLANE) + at + g * 4, 4) if c == 0 else pl.ds(g * PLANE + at + q * 4, 4)
                        rows = (first, pl.ds(256 + at + zz * 4 + y, 4, stride=PLANE), pl.ds(512 + at + y * PLANE + zz, 4, stride=4))
                    xc_ref[2 * c + b, rows[r // 2], :] = v
    each_plane(place, rb_ref, esem, put)


def finish_rows(place, rb_ref, esem, um1_ref, um2_ref, y_ref):
    def put(c, q, g, x):
        f = dotf(um1_ref[...] if c == 1 else um2_ref[...], x)
        for b in PAIR:
            for r in range(6):
                at = (b * 6 + r) * 8
                if c == 1:
                    for core in PAIR:
                        rows = pl.ds(g * 192 + q * 12 + core * 6 + r, 4, stride=48)
                        y_ref[2 * c + b, rows, :] = y_ref[2 * c + b, rows, :] + f[at + core * 4:at + core * 4 + 4]
                else:
                    rows = pl.ds((q * SIDE + g * 8) * 6 + r if c == 0 else (g * SIDE + q * 8) * 6 + r, 8, stride=6)
                    y_ref[2 * c + b, rows, :] = y_ref[2 * c + b, rows, :] + f[at:at + 8]
    each_plane(place, rb_ref, esem, put)


def stage(end, place, gather, heads, xc_ref, b_ref, gb_ref, w_ref, wb_ref, wo_ref, w1_ref, w2_ref, bm_ref, pm_ref, y_ref, rb_ref, esem, fsem,
          u_ref, q_ref, g_ref, kT_ref, v_ref, bf_ref, hb_ref, sb_ref, s_refs, p_refs, wkT_ref, entry_wait):
    per, n, c = xc_ref.shape
    hd = c // heads
    nq = n // 4
    scale = hd ** -0.5 * LOG2E
    me = place.me

    wb = wb_ref[...].astype(F32)
    none = jnp.zeros_like(wb)
    wide = [jnp.concatenate(p, axis=0).astype(BF16) for p in ((wb, none), (none, wb))]

    def bias_rows(col, _):
        acc = None
        for r2 in PAIR:
            i = col * 2 + r2
            u = ln(xc_ref[i])
            u_ref[i] = u
            t = dot_nt(wide[r2], u)
            acc = t if acc is None else acc + t
        b_ref[col] = acc.astype(BF16)
        for k in COLOURS:
            @pl.when(col == k)
            def _():
                if k == 0 and not end:
                    entry_wait()
                gather.first(k)
        return 0
    lax.fori_loop(0, 3, bias_rows, 0)

    wkT_ref[...] = w_ref[:, c:2 * c].T

    def project(i):
        u = u_ref[i]
        kT_ref[i] = dot_nt(wkT_ref[...], u).astype(BF16)
        q_ref[i] = dotf(u, w_ref[:, :c]).astype(BF16)
        vg = dotf(u, w_ref[:, 2 * c:])
        v_ref[i, :, :c] = vg[:, :c].astype(BF16)
        if not end:
            v_ref[i, :, c:] = jnp.ones((n, c), BF16)
        g_ref[i] = jax.nn.sigmoid(vg[:, c:])

    def prepare(i, _):
        project(i)
        for col in COLOURS:
            @pl.when(i == col)
            def _():
                gather.second(col)

            @pl.when(i == col + 3)
            def _():
                gather.third(col)
        return 0
    lax.fori_loop(0, per, prepare, 0)

    order = (0, 3, 1, 2)

    def pick(step):
        return jnp.where(step == 1, 3, jnp.where(step == 2, 1, jnp.where(step == 3, 2, 0)))

    def send(col, plane, o, step):
        k = lax.rem(slot_of(col, place), SIDE) ^ o
        rcopy(sb_ref.at[col, plane * SIDE + k], rb_ref.at[col, inbox(col, place)], fsem, esem.at[step], dest_of(col, plane, k)).start()

    def finish_block(t):
        if not end:
            store_rows(place, y_ref, hb_ref, t)

    def block(step, _):
        first = isinstance(step, int)
        t = 0 if first else pick(step)
        before = None if first else [place.plane(col, pick(step - 1)) for col in COLOURS]
        gather.partner_wait(5 + step)
        planes = [place.plane(col, t) for col in COLOURS]
        for col in COLOURS:
            b = gb_ref[col, pl.ds(mult(planes[col] * SIDE, SIDE), SIDE)].reshape(256, n)
            f = dotf(bm_ref[...], b) * LOG2E
            for h in range(heads):
                bf_ref[h * nq + col * PLANE:h * nq + (col + 1) * PLANE, :] = f[h * PLANE:(h + 1) * PLANE]
        rows = [pl.ds(mult(col * 256 + planes[col] * PLANE, PLANE), PLANE) for col in COLOURS]

        lane = lax.broadcasted_iota(jnp.int32, (nq, c), 1) // hd

        def scores(i):
            qb = jnp.concatenate([q_ref[i, r, :] for r in rows], axis=0)
            qm = jnp.concatenate([jnp.where(lane == h, qb, jnp.zeros_like(qb)) for h in range(heads)], axis=0)
            s_refs[i % 2][...] = dotf(qm, kT_ref[i]) * scale + bf_ref[...]

        def soften(i):
            t = s_refs[i % 2][...]
            m = jnp.max(t, axis=-1, keepdims=True)
            p_refs[i % 2][...] = jnp.exp2(t - m).astype(BF16)

        def mix(i):
            o = dotf(p_refs[i % 2][...], v_ref[i])
            o = o[:, :c] / o[:, c:]
            res = jnp.zeros((nq, c), F32)
            for h in range(heads):
                res = jnp.where(lane == h, o[h * nq:(h + 1) * nq], res)
            og = (res * jnp.concatenate([g_ref[i, r, :] for r in rows], axis=0)).astype(BF16)
            upd = dotf(og, wo_ref[...])
            if end:
                hb_ref[i] = upd
            else:
                hb_ref[i] = jnp.concatenate([xc_ref[i, r, :] for r in rows], axis=0) + upd

        if not first:
            @pl.when(step > 1)
            def _():
                for col in COLOURS:
                    send(col, before[col], 0, step - 1)
        scores(0)
        for i in range(per):
            if not first:
                for o in range(1 + i * 31 // per, 1 + (i + 1) * 31 // per):
                    for col in COLOURS:
                        send(col, before[col], o, step - 1)
            if i + 1 < per:
                scores(i + 1)
            soften(i)
            if i > 0:
                mix(i - 1)
        mix(per - 1)
        if first:
            gather.forward()
        else:
            @pl.when(step == 1)
            def _():
                gather.last()

        if end:
            def trans(i, _):
                upd = jnp.concatenate([hb_ref[2 * i], hb_ref[2 * i + 1]], axis=0)
                two = jnp.concatenate([xc_ref[2 * i + a, r, :] for a in PAIR for r in rows], axis=0) + upd
                hid = jnp.maximum(dotf(ln(two), w1_ref[...]), 0).astype(BF16)
                new = upd + dotf(hid, w2_ref[...])
                hb_ref[2 * i] = new[:nq]
                hb_ref[2 * i + 1] = new[nq:]
                return 0
            lax.fori_loop(0, per // 2, trans, 0, unroll=3)
        def pack(kg, _):
            for col in COLOURS:
                x = jnp.concatenate([hb_ref[i, pl.ds(mult(col * PLANE + r2 * SIDE + kg * 8, 8), 8), :] for i in range(per) for r2 in PAIR], axis=0)
                f = dotf(pm_ref[...], x.astype(BF16)).reshape(8, 12, c).astype(BF16)
                sb_ref[col, pl.ds(mult(planes[col] * SIDE + kg * 8, 8), 8)] = f
            return 0
        lax.fori_loop(0, 4, pack, 0, unroll=4)
        if first:
            finish_block(0)
        else:
            @pl.when(step < 3)
            def _():
                finish_block(t)

        return 0

    block(0, 0)
    lax.fori_loop(1, 4, block, 0)
    tail = [place.plane(col, order[3]) for col in COLOURS]

    def send_tail(o, _):
        for col in COLOURS:
            send(col, tail[col], o, 3)
        return 0
    lax.fori_loop(0, SIDE, send_tail, 0)
    finish_block(order[3])
    for col in COLOURS:
        rb_ref[col, inbox(col, place)] = sb_ref[col, slot_of(col, place)]


def drain(gather, rb_ref, fsem):
    gather.drain()
    bytes_wait(rb_ref.at[:, pl.ds(0, 127)], fsem)


def kernel(heads, devs, z_ref, ws_ref, wbs_ref, wos_ref, we_ref, wbe_ref, woe_ref, w1_ref, w2_ref, bm_ref, pm_ref, um1_ref, um2_ref, y_ref,
           xc_ref, b_ref, gb1_ref, gb2_ref, rb1_ref, rb2_ref, u_ref, q_ref, g_ref, kT_ref, v_ref, bf_ref, hb_ref, sb_ref, sa_ref, sb2_ref, pa_ref, pb_ref, wkT_ref,
           gs1, gr1, gs2, gr2, e1, f1, e2, f2):
    place = Place()
    barrier = pltpu.get_barrier_semaphore()

    def greet(k, _):
        pl.semaphore_signal(barrier, inc=1, device_id={'sp': place.me ^ k}, device_id_type=MESH)
        return 0
    lax.fori_loop(1, devs, greet, 0)

    def entry_wait():
        pl.semaphore_wait(barrier, devs - 1)
    work = (u_ref, q_ref, g_ref, kT_ref, v_ref, bf_ref, hb_ref, sb_ref, (sa_ref, sb2_ref), (pa_ref, pb_ref), wkT_ref, entry_wait)
    load_rows(z_ref, xc_ref)
    gather = Gather(place, b_ref.at[0], gb1_ref, gs1, gr1)
    stage(False, place, gather, heads, xc_ref, b_ref.at[0], gb1_ref, ws_ref, wbs_ref, wos_ref, w1_ref, w2_ref,
          bm_ref, pm_ref, y_ref, rb1_ref, e1, f1, *work)
    receive_rows(place, rb1_ref, e1, um1_ref, xc_ref)
    drain(gather, rb1_ref, f1)
    gather = Gather(place, b_ref.at[1], gb2_ref, gs2, gr2)
    stage(True, place, gather, heads, xc_ref, b_ref.at[1], gb2_ref, we_ref, wbe_ref, woe_ref, w1_ref, w2_ref,
          bm_ref, pm_ref, y_ref, rb2_ref, e2, f2, *work)
    finish_rows(place, rb2_ref, e2, um1_ref, um2_ref, y_ref)
    drain(gather, rb2_ref, f2)


def pack_matrix():
    m = np.zeros((8, 12, 6, 2, 8), np.float32)
    for k in range(8):
        for i in range(6):
            for r in PAIR:
                m[k, i * 2 + r, i, r, k] = 1
    return jnp.asarray(m.reshape(96, 96), BF16)


def unpack_matrix(swap):
    m = np.zeros((2, 6, 8, 8, 12), np.float32)
    for k in range(8):
        for i in range(6):
            for r in PAIR:
                row = (k % 2) * 4 + k // 2 if swap else k
                m[r, i, row, k, i * 2 + r] = 1
    return jnp.asarray(m.reshape(96, 96), BF16)


def bias_matrix(heads):
    m = np.zeros((heads, 2, SIDE, SIDE, 2, heads), np.float32)
    for k in range(SIDE):
        for r in PAIR:
            for h in range(heads):
                m[h, r, k, k, r, h] = 1
    return jnp.asarray(m.reshape(256, 256), BF16)


def solution(mesh):
    devs = mesh.shape['sp']
    row_spec = P(('dp', 'sp'), None, None)
    vmem = pl.BlockSpec(memory_space=pltpu.VMEM)
    dma = pltpu.SemaphoreType.DMA

    def local_fn(z, wqkvg_s, wb_s, wo_s, wqkvg_e, wb_e, wo_e, w1, w2):
        per, n, c = z.shape
        heads = wb_s.shape[0]
        args = (z, wqkvg_s, wb_s, wo_s, wqkvg_e, wb_e, wo_e, w1, w2, bias_matrix(heads), pack_matrix(), unpack_matrix(True), unpack_matrix(False))
        return pl.pallas_call(
            functools.partial(kernel, heads, devs), in_specs=[vmem] * len(args), out_specs=vmem,
            out_shape=jax.ShapeDtypeStruct(z.shape, F32),
            scratch_shapes=[
                pltpu.VMEM((per, n, c), F32), pltpu.VMEM((2, 3, 8, n), BF16),
                pltpu.VMEM((3, devs, 8, n), BF16), pltpu.VMEM((3, devs, 8, n), BF16),
                pltpu.VMEM((3, devs, 12, c), BF16), pltpu.VMEM((3, devs, 12, c), BF16),
                pltpu.VMEM((per, n, c), BF16), pltpu.VMEM((per, n, c), BF16), pltpu.VMEM((per, n, c), F32),
                pltpu.VMEM((per, c, n), BF16), pltpu.VMEM((per, n, 2 * c), BF16), pltpu.VMEM((heads * n // 4, n), F32),
                pltpu.VMEM((per, n // 4, c), F32), pltpu.VMEM((3, devs, 12, c), BF16),
                pltpu.VMEM((heads * n // 4, n), F32), pltpu.VMEM((heads * n // 4, n), F32),
                pltpu.VMEM((heads * n // 4, n), BF16), pltpu.VMEM((heads * n // 4, n), BF16),
                pltpu.VMEM((c, c), BF16),
                dma, dma((3, 9)), dma, dma((3, 9)), dma((4,)), dma, dma((4,)), dma],
            compiler_params=pltpu.CompilerParams(has_side_effects=True, collective_id=0, vmem_limit_bytes=60 * 2**20), name='block')(*args)

    return jax.shard_map(local_fn, mesh=mesh, in_specs=(row_spec,) + (P(),) * 8, out_specs=row_spec, check_vma=False)
```

```python
import functools
import math
import jax
import jax.numpy as jnp
import numpy as np
from jax import lax
from jax.experimental import pallas as pl
from jax.experimental.pallas import tpu as pltpu
from jax.sharding import PartitionSpec as P

F32, BF16 = jnp.float32, jnp.bfloat16
MESH = pl.DeviceIdType.MESH
LOG2E = math.log2(math.e)
EPS = 1e-5
X, Y, Z = 0, 1, 2
COLOURS = range(3)
PAIR = range(2)
QUAD = range(4)
HALF, SIDE, PLANE = 16, 32, 64
DEV = (2, 8, 32)
DIMS = ((X, Y, Z), (Y, Z, X), (Z, X, Y))
SLOT = ((1, 4, 32), (32, 1, 4), (4, 32, 1))


def ln(x):
    mu = jnp.mean(x, axis=-1, keepdims=True)
    c = x - mu
    var = jnp.mean(c * c, axis=-1, keepdims=True)
    return (c * lax.rsqrt(var + EPS)).astype(BF16)


def dotf(a, b):
    return jnp.dot(a, b, preferred_element_type=F32)


def dot_nt(a, b):
    return lax.dot_general(a, b, (((1,), (1,)), ((), ())), preferred_element_type=F32)


def mult(v, k):
    return pl.multiple_of(v, k)


def rcopy(src, dst, ssem, rsem, peer):
    return pltpu.make_async_remote_copy(src_ref=src, dst_ref=dst, send_sem=ssem, recv_sem=rsem, device_id={'sp': peer}, device_id_type=MESH)


def bytes_wait(ref, sem):
    pltpu.make_async_copy(ref, ref, sem).wait()


class Place:
    def __init__(self):
        self.me = lax.axis_index('sp')
        self.core = lax.rem(self.me, 2)
        self.at = [lax.rem(self.me // s, 4) for s in DEV]

    def ring(self, dim, t):
        return self.me + (lax.rem(self.at[dim] + t, 4) - self.at[dim]) * DEV[dim]

    def plane(self, c, t):
        return lax.rem(self.at[DIMS[c][2]] + t, 4)


def slot_of(c, place):
    return place.core * HALF + sum(place.at[d] * SLOT[c][d] for d in COLOURS)


def dest_of(c, plane, k):
    if c == 0:
        return plane * SIDE + lax.rem(k, HALF) * 2 + k // HALF
    if c == 1:
        return lax.rem(k, HALF) * 8 + plane * 2 + k // HALF
    return lax.rem(k, 4) * SIDE + plane * 8 + lax.rem(k // 4, 4) * 2 + k // HALF


class Gather:
    def __init__(self, place, b_ref, g_ref, ssem, rsem):
        self.p, self.b, self.g, self.ssem, self.rsem = place, b_ref, g_ref, ssem, rsem

    def push(self, c, start, count, peer, k):
        part = self.g.at[c, pl.ds(start, count)]
        rcopy(part, part, self.ssem, self.rsem.at[c, k], peer).start()

    def half(self, c, t):
        return self.p.plane(c, t) * SIDE + self.p.core * HALF

    def first(self, c):
        p = self.p
        slot = slot_of(c, p)
        for t in (1, 3, 2):
            rcopy(self.b.at[c], self.g.at[c, slot], self.ssem, self.rsem.at[c, 0], p.ring(DIMS[c][0], t)).start()
        self.g[c, slot] = self.b[c]

    def second(self, c):
        p = self.p
        b = DIMS[c][1]
        bytes_wait(self.g.at[c, pl.ds(0, 3)], self.rsem.at[c, 0])
        for t in (1, 3, 2):
            self.push(c, self.half(c, 0) + p.at[b] * 4, 4, p.ring(b, t), 1)

    def third(self, c):
        p = self.p
        d = DIMS[c][2]
        bytes_wait(self.g.at[c, pl.ds(0, 12)], self.rsem.at[c, 1])
        self.push(c, self.half(c, 0), HALF, p.me ^ 1, 5)
        self.push(c, self.half(c, 0), HALF, p.ring(d, 1), 2)
        self.push(c, self.half(c, 0), HALF, p.ring(d, 3), 3)

    def forward(self):
        p = self.p
        for side, t in ((0, 3), (1, 1)):
            for c in COLOURS:
                bytes_wait(self.g.at[c, pl.ds(0, HALF)], self.rsem.at[c, 2 + side])
                self.push(c, self.half(c, t), HALF, p.me ^ 1, 6 + 2 * side)
                self.push(c, self.half(c, t) + side * 8, 8, p.ring(DIMS[c][2], 4 - t), 4)

    def last(self):
        for c in COLOURS:
            bytes_wait(self.g.at[c, pl.ds(0, HALF)], self.rsem.at[c, 4])
            self.push(c, self.half(c, 2), HALF, self.p.me ^ 1, 7)

    def partner_wait(self, k):
        for c in COLOURS:
            bytes_wait(self.g.at[c, pl.ds(0, HALF)], self.rsem.at[c, k])

    def drain(self):
        for c in COLOURS:
            bytes_wait(self.g.at[c, pl.ds(0, 127)], self.ssem)


def load_rows(z_ref, xc_ref):
    def body(i, _):
        for r2 in PAIR:
            for p in QUAD:
                for core in PAIR:
                    at = p * PLANE + r2 * SIDE + core * HALF
                    xc_ref[i, pl.ds(at, HALF), :] = z_ref[i, pl.ds((p * SIDE + core) * 6 + r2, HALF, stride=12), :]
                    xc_ref[i, pl.ds(256 + at, HALF), :] = z_ref[i, pl.ds((p * 2 + core) * 6 + 2 + r2, HALF, stride=48), :]
                    for x in QUAD:
                        xc_ref[i, pl.ds(512 + at + x * 4, 4), :] = z_ref[i, pl.ds((p * 8 + x * 2 + core) * 6 + 4 + r2, 4, stride=192), :]
        return 0
    lax.fori_loop(0, z_ref.shape[0], body, 0)


def store_rows(place, y_ref, hb_ref, t):
    def body(i, _):
        p0, p1, p2 = (place.plane(c, t) for c in COLOURS)
        for r2 in PAIR:
            for core in PAIR:
                at = r2 * SIDE + core * HALF
                y_ref[i, pl.ds(p0 * 192 + core * 6 + r2, HALF, stride=12), :] = hb_ref[i, pl.ds(at, HALF), :]
                y_ref[i, pl.ds(p1 * 12 + core * 6 + 2 + r2, HALF, stride=48), :] = hb_ref[i, pl.ds(PLANE + at, HALF), :]
                for x in QUAD:
                    y_ref[i, pl.ds(p2 * 48 + x * 12 + core * 6 + 4 + r2, 4, stride=192), :] = hb_ref[i, pl.ds(128 + at + x * 4, 4), :]
        return 0
    lax.fori_loop(0, y_ref.shape[0], body, 0)


def inbox(c, place):
    x, y, z = place.at
    if c == 0:
        return place.me
    if c == 1:
        return x * SIDE + z * 8 + y * 2 + place.core
    return y * SIDE + z * 8 + x * 2 + place.core


def each_plane(place, rb_ref, esem, fn):
    def body(step, _):
        @pl.when(step == 0)
        def _():
            bytes_wait(rb_ref.at[:, pl.ds(0, 31)], esem.at[step])

        @pl.when(step > 0)
        def _():
            bytes_wait(rb_ref.at[:, pl.ds(0, SIDE)], esem.at[step])
        for c in COLOURS:
            q = place.plane(c, step)
            for g in QUAD:
                fn(c, q, g, rb_ref[c, pl.ds(mult(q * SIDE + g * 8, 8), 8)].reshape(96, 128))
        return 0
    lax.fori_loop(0, 4, body, 0)


def receive_rows(place, rb_ref, esem, um_ref, xc_ref):
    def put(c, q, g, x):
        f = dotf(um_ref[...], x)
        for b in PAIR:
            for r in range(6):
                for core in PAIR:
                    v = f[(b * 6 + r) * 8 + core * 4:(b * 6 + r) * 8 + core * 4 + 4]
                    at = (r % 2) * SIDE + core * HALF
                    if c == 1:
                        rows = (pl.ds(g * PLANE + at + q, 4, stride=4), pl.ds(mult(q * PLANE, PLANE) + 256 + at + g * 4, 4), pl.ds(512 + at + q * 4 + g, 4, stride=PLANE))
                    else:
                        zz, y = (q, g) if c == 0 else (g, q)
                        first = pl.ds(mult(q * PLANE, PLANE) + at + g * 4, 4) if c == 0 else pl.ds(g * PLANE + at + q * 4, 4)
                        rows = (first, pl.ds(256 + at + zz * 4 + y, 4, stride=PLANE), pl.ds(512 + at + y * PLANE + zz, 4, stride=4))
                    xc_ref[2 * c + b, rows[r // 2], :] = v
    each_plane(place, rb_ref, esem, put)


def finish_rows(place, rb_ref, esem, um1_ref, um2_ref, y_ref):
    def put(c, q, g, x):
        f = dotf(um1_ref[...] if c == 1 else um2_ref[...], x)
        for b in PAIR:
            for r in range(6):
                at = (b * 6 + r) * 8
                if c == 1:
                    for core in PAIR:
                        rows = pl.ds(g * 192 + q * 12 + core * 6 + r, 4, stride=48)
                        y_ref[2 * c + b, rows, :] = y_ref[2 * c + b, rows, :] + f[at + core * 4:at + core * 4 + 4]
                else:
                    rows = pl.ds((q * SIDE + g * 8) * 6 + r if c == 0 else (g * SIDE + q * 8) * 6 + r, 8, stride=6)
                    y_ref[2 * c + b, rows, :] = y_ref[2 * c + b, rows, :] + f[at:at + 8]
    each_plane(place, rb_ref, esem, put)


def stage(end, place, gather, heads, xc_ref, b_ref, gb_ref, w_ref, wb_ref, wo_ref, w1_ref, w2_ref, bm_ref, pm_ref, y_ref, rb_ref, esem, fsem,
          u_ref, q_ref, g_ref, kT_ref, v_ref, bf_ref, hb_ref, sb_ref, s_refs, p_refs, wkT_ref, entry_wait):
    per, n, c = xc_ref.shape
    hd = c // heads
    nq = n // 4
    scale = hd ** -0.5 * LOG2E
    me = place.me

    wb = wb_ref[...].astype(F32)
    none = jnp.zeros_like(wb)
    wide = [jnp.concatenate(p, axis=0).astype(BF16) for p in ((wb, none), (none, wb))]

    def bias_rows(col, _):
        acc = None
        for r2 in PAIR:
            i = col * 2 + r2
            u = ln(xc_ref[i])
            u_ref[i] = u
            t = dot_nt(wide[r2], u)
            acc = t if acc is None else acc + t
        b_ref[col] = acc.astype(BF16)
        for k in COLOURS:
            @pl.when(col == k)
            def _():
                if k == 0 and not end:
                    entry_wait()
                gather.first(k)
        return 0
    lax.fori_loop(0, 3, bias_rows, 0)

    wkT_ref[...] = w_ref[:, c:2 * c].T

    def project(i):
        u = u_ref[i]
        kT_ref[i] = dot_nt(wkT_ref[...], u).astype(BF16)
        q_ref[i] = dotf(u, w_ref[:, :c]).astype(BF16)
        vg = dotf(u, w_ref[:, 2 * c:])
        v_ref[i, :, :c] = vg[:, :c].astype(BF16)
        if not end:
            v_ref[i, :, c:] = jnp.ones((n, c), BF16)
        g_ref[i] = jax.nn.sigmoid(vg[:, c:])

    def prepare(i, _):
        project(i)
        for col in COLOURS:
            @pl.when(i == col)
            def _():
                gather.second(col)

            @pl.when(i == col + 3)
            def _():
                gather.third(col)
        return 0
    lax.fori_loop(0, per, prepare, 0)

    order = (0, 3, 2, 1)

    def pick(step):
        return lax.rem(4 - step, 4)

    def send(col, plane, o, step):
        k = lax.rem(slot_of(col, place), SIDE) ^ o
        rcopy(sb_ref.at[col, plane * SIDE + k], rb_ref.at[col, inbox(col, place)], fsem, esem.at[step], dest_of(col, plane, k)).start()

    def finish_block(t):
        if not end:
            store_rows(place, y_ref, hb_ref, t)

    def block(step, _):
        first = isinstance(step, int)
        t = 0 if first else pick(step)
        before = None if first else [place.plane(col, pick(step - 1)) for col in COLOURS]
        gather.partner_wait(5 + step)
        planes = [place.plane(col, t) for col in COLOURS]
        for col in COLOURS:
            b = gb_ref[col, pl.ds(mult(planes[col] * SIDE, SIDE), SIDE)].reshape(256, n)
            f = dotf(bm_ref[...], b) * LOG2E
            for h in range(heads):
                bf_ref[h * nq + col * PLANE:h * nq + (col + 1) * PLANE, :] = f[h * PLANE:(h + 1) * PLANE]
        rows = [pl.ds(mult(col * 256 + planes[col] * PLANE, PLANE), PLANE) for col in COLOURS]

        lane = lax.broadcasted_iota(jnp.int32, (nq, c), 1) // hd

        def scores(i):
            qb = jnp.concatenate([q_ref[i, r, :] for r in rows], axis=0)
            qm = jnp.concatenate([jnp.where(lane == h, qb, jnp.zeros_like(qb)) for h in range(heads)], axis=0)
            s_refs[i % 2][...] = dotf(qm, kT_ref[i]) * scale + bf_ref[...]

        def soften(i):
            t = s_refs[i % 2][...]
            m = jnp.max(t, axis=-1, keepdims=True)
            p_refs[i % 2][...] = jnp.exp2(t - m).astype(BF16)

        def mix(i):
            o = dotf(p_refs[i % 2][...], v_ref[i])
            o = o[:, :c] / o[:, c:]
            res = jnp.zeros((nq, c), F32)
            for h in range(heads):
                res = jnp.where(lane == h, o[h * nq:(h + 1) * nq], res)
            og = (res * jnp.concatenate([g_ref[i, r, :] for r in rows], axis=0)).astype(BF16)
            upd = dotf(og, wo_ref[...])
            if end:
                hb_ref[i] = upd
            else:
                hb_ref[i] = jnp.concatenate([xc_ref[i, r, :] for r in rows], axis=0) + upd

        if not first:
            @pl.when(step > 1)
            def _():
                for col in COLOURS:
                    send(col, before[col], 0, step - 1)
        scores(0)
        for i in range(per):
            if not first:
                for o in range(1 + i * 31 // per, 1 + (i + 1) * 31 // per):
                    for col in COLOURS:
                        send(col, before[col], o, step - 1)
            if i + 1 < per:
                scores(i + 1)
            soften(i)
            if i > 0:
                mix(i - 1)
        mix(per - 1)
        if first:
            gather.forward()
        else:
            @pl.when(step == 1)
            def _():
                gather.last()

        if end:
            def trans(i, _):
                upd = jnp.concatenate([hb_ref[2 * i], hb_ref[2 * i + 1]], axis=0)
                two = jnp.concatenate([xc_ref[2 * i + a, r, :] for a in PAIR for r in rows], axis=0) + upd
                hid = jnp.maximum(dotf(ln(two), w1_ref[...]), 0).astype(BF16)
                new = upd + dotf(hid, w2_ref[...])
                hb_ref[2 * i] = new[:nq]
                hb_ref[2 * i + 1] = new[nq:]
                return 0
            lax.fori_loop(0, per // 2, trans, 0, unroll=3)
        def pack(kg, _):
            for col in COLOURS:
                x = jnp.concatenate([hb_ref[i, pl.ds(mult(col * PLANE + r2 * SIDE + kg * 8, 8), 8), :] for i in range(per) for r2 in PAIR], axis=0)
                f = dotf(pm_ref[...], x.astype(BF16)).reshape(8, 12, c).astype(BF16)
                sb_ref[col, pl.ds(mult(planes[col] * SIDE + kg * 8, 8), 8)] = f
            return 0
        lax.fori_loop(0, 4, pack, 0, unroll=4)
        if first:
            finish_block(0)
        else:
            @pl.when(step < 3)
            def _():
                finish_block(t)

        return 0

    block(0, 0)
    lax.fori_loop(1, 4, block, 0)
    tail = [place.plane(col, order[3]) for col in COLOURS]

    def send_tail(o, _):
        for col in COLOURS:
            send(col, tail[col], o, 3)
        return 0
    lax.fori_loop(0, SIDE, send_tail, 0)
    finish_block(order[3])
    for col in COLOURS:
        rb_ref[col, inbox(col, place)] = sb_ref[col, slot_of(col, place)]


def drain(gather, rb_ref, fsem):
    gather.drain()
    bytes_wait(rb_ref.at[:, pl.ds(0, 127)], fsem)


def kernel(heads, devs, z_ref, ws_ref, wbs_ref, wos_ref, we_ref, wbe_ref, woe_ref, w1_ref, w2_ref, bm_ref, pm_ref, um1_ref, um2_ref, y_ref,
           xc_ref, b_ref, gb1_ref, gb2_ref, rb1_ref, rb2_ref, u_ref, q_ref, g_ref, kT_ref, v_ref, bf_ref, hb_ref, sb_ref, sa_ref, sb2_ref, pa_ref, pb_ref, wkT_ref,
           gs1, gr1, gs2, gr2, e1, f1, e2, f2):
    place = Place()
    barrier = pltpu.get_barrier_semaphore()

    friends = [place.me ^ 1] + [place.ring(d, t) for d in COLOURS for t in QUAD if t]
    for peer in friends:
        pl.semaphore_signal(barrier, inc=1, device_id={'sp': peer}, device_id_type=MESH)

    def entry_wait():
        pl.semaphore_wait(barrier, len(friends))
    work = (u_ref, q_ref, g_ref, kT_ref, v_ref, bf_ref, hb_ref, sb_ref, (sa_ref, sb2_ref), (pa_ref, pb_ref), wkT_ref, entry_wait)
    load_rows(z_ref, xc_ref)
    gather = Gather(place, b_ref.at[0], gb1_ref, gs1, gr1)
    stage(False, place, gather, heads, xc_ref, b_ref.at[0], gb1_ref, ws_ref, wbs_ref, wos_ref, w1_ref, w2_ref,
          bm_ref, pm_ref, y_ref, rb1_ref, e1, f1, *work)
    receive_rows(place, rb1_ref, e1, um1_ref, xc_ref)
    drain(gather, rb1_ref, f1)
    gather = Gather(place, b_ref.at[1], gb2_ref, gs2, gr2)
    stage(True, place, gather, heads, xc_ref, b_ref.at[1], gb2_ref, we_ref, wbe_ref, woe_ref, w1_ref, w2_ref,
          bm_ref, pm_ref, y_ref, rb2_ref, e2, f2, *work)
    finish_rows(place, rb2_ref, e2, um1_ref, um2_ref, y_ref)
    drain(gather, rb2_ref, f2)


def pack_matrix():
    m = np.zeros((8, 12, 6, 2, 8), np.float32)
    for k in range(8):
        for i in range(6):
            for r in PAIR:
                m[k, i * 2 + r, i, r, k] = 1
    return jnp.asarray(m.reshape(96, 96), BF16)


def unpack_matrix(swap):
    m = np.zeros((2, 6, 8, 8, 12), np.float32)
    for k in range(8):
        for i in range(6):
            for r in PAIR:
                row = (k % 2) * 4 + k // 2 if swap else k
                m[r, i, row, k, i * 2 + r] = 1
    return jnp.asarray(m.reshape(96, 96), BF16)


def bias_matrix(heads):
    m = np.zeros((heads, 2, SIDE, SIDE, 2, heads), np.float32)
    for k in range(SIDE):
        for r in PAIR:
            for h in range(heads):
                m[h, r, k, k, r, h] = 1
    return jnp.asarray(m.reshape(256, 256), BF16)


def solution(mesh):
    devs = mesh.shape['sp']
    row_spec = P(('dp', 'sp'), None, None)
    vmem = pl.BlockSpec(memory_space=pltpu.VMEM)
    dma = pltpu.SemaphoreType.DMA

    def local_fn(z, wqkvg_s, wb_s, wo_s, wqkvg_e, wb_e, wo_e, w1, w2):
        per, n, c = z.shape
        heads = wb_s.shape[0]
        args = (z, wqkvg_s, wb_s, wo_s, wqkvg_e, wb_e, wo_e, w1, w2, bias_matrix(heads), pack_matrix(), unpack_matrix(True), unpack_matrix(False))
        return pl.pallas_call(
            functools.partial(kernel, heads, devs), in_specs=[vmem] * len(args), out_specs=vmem,
            out_shape=jax.ShapeDtypeStruct(z.shape, F32),
            scratch_shapes=[
                pltpu.VMEM((per, n, c), F32), pltpu.VMEM((2, 3, 8, n), BF16),
                pltpu.VMEM((3, devs, 8, n), BF16), pltpu.VMEM((3, devs, 8, n), BF16),
                pltpu.VMEM((3, devs, 12, c), BF16), pltpu.VMEM((3, devs, 12, c), BF16),
                pltpu.VMEM((per, n, c), BF16), pltpu.VMEM((per, n, c), BF16), pltpu.VMEM((per, n, c), F32),
                pltpu.VMEM((per, c, n), BF16), pltpu.VMEM((per, n, 2 * c), BF16), pltpu.VMEM((heads * n // 4, n), F32),
                pltpu.VMEM((per, n // 4, c), F32), pltpu.VMEM((3, devs, 12, c), BF16),
                pltpu.VMEM((heads * n // 4, n), F32), pltpu.VMEM((heads * n // 4, n), F32),
                pltpu.VMEM((heads * n // 4, n), BF16), pltpu.VMEM((heads * n // 4, n), BF16),
                pltpu.VMEM((c, c), BF16),
                dma, dma((3, 9)), dma, dma((3, 9)), dma((4,)), dma, dma((4,)), dma],
            compiler_params=pltpu.CompilerParams(has_side_effects=True, collective_id=0, vmem_limit_bytes=60 * 2**20), name='block')(*args)

    return jax.shard_map(local_fn, mesh=mesh, in_specs=(row_spec,) + (P(),) * 8, out_specs=row_spec, check_vma=False)
```

```python
import functools
import math
import jax
import jax.numpy as jnp
import numpy as np
from jax import lax
from jax.experimental import pallas as pl
from jax.experimental.pallas import tpu as pltpu
from jax.sharding import PartitionSpec as P

F32, BF16 = jnp.float32, jnp.bfloat16
MESH = pl.DeviceIdType.MESH
LOG2E = math.log2(math.e)
EPS = 1e-5
X, Y, Z = 0, 1, 2
COLOURS = range(3)
PAIR = range(2)
QUAD = range(4)
HALF, SIDE, PLANE = 16, 32, 64
DEV = (2, 8, 32)
DIMS = ((X, Y, Z), (Y, Z, X), (Z, X, Y))
SLOT = ((1, 4, 32), (32, 1, 4), (4, 32, 1))


def ln(x):
    mu = jnp.mean(x, axis=-1, keepdims=True)
    c = x - mu
    var = jnp.mean(c * c, axis=-1, keepdims=True)
    return (c * lax.rsqrt(var + EPS)).astype(BF16)


def dotf(a, b):
    return jnp.dot(a, b, preferred_element_type=F32)


def dot_nt(a, b):
    return lax.dot_general(a, b, (((1,), (1,)), ((), ())), preferred_element_type=F32)


def mult(v, k):
    return pl.multiple_of(v, k)


def rcopy(src, dst, ssem, rsem, peer):
    return pltpu.make_async_remote_copy(src_ref=src, dst_ref=dst, send_sem=ssem, recv_sem=rsem, device_id={'sp': peer}, device_id_type=MESH)


def bytes_wait(ref, sem):
    pltpu.make_async_copy(ref, ref, sem).wait()


class Place:
    def __init__(self):
        self.me = lax.axis_index('sp')
        self.core = lax.rem(self.me, 2)
        self.at = [lax.rem(self.me // s, 4) for s in DEV]

    def ring(self, dim, t):
        return self.me + (lax.rem(self.at[dim] + t, 4) - self.at[dim]) * DEV[dim]

    def plane(self, c, t):
        return lax.rem(self.at[DIMS[c][2]] + t, 4)


def slot_of(c, place):
    return place.core * HALF + sum(place.at[d] * SLOT[c][d] for d in COLOURS)


def dest_of(c, plane, k):
    if c == 0:
        return plane * SIDE + lax.rem(k, HALF) * 2 + k // HALF
    if c == 1:
        return lax.rem(k, HALF) * 8 + plane * 2 + k // HALF
    return lax.rem(k, 4) * SIDE + plane * 8 + lax.rem(k // 4, 4) * 2 + k // HALF


class Gather:
    def __init__(self, place, b_ref, g_ref, ssem, rsem):
        self.p, self.b, self.g, self.ssem, self.rsem = place, b_ref, g_ref, ssem, rsem

    def push(self, c, start, count, peer, k):
        part = self.g.at[c, pl.ds(start, count)]
        rcopy(part, part, self.ssem, self.rsem.at[c, k], peer).start()

    def half(self, c, t):
        return self.p.plane(c, t) * SIDE + self.p.core * HALF

    def first(self, c):
        p = self.p
        slot = slot_of(c, p)
        for t in (1, 3, 2):
            rcopy(self.b.at[c], self.g.at[c, slot], self.ssem, self.rsem.at[c, 0], p.ring(DIMS[c][0], t)).start()
        self.g[c, slot] = self.b[c]

    def second(self, c):
        p = self.p
        b = DIMS[c][1]
        bytes_wait(self.g.at[c, pl.ds(0, 3)], self.rsem.at[c, 0])
        for t in (1, 3, 2):
            self.push(c, self.half(c, 0) + p.at[b] * 4, 4, p.ring(b, t), 1)

    def third(self, c):
        p = self.p
        d = DIMS[c][2]
        bytes_wait(self.g.at[c, pl.ds(0, 12)], self.rsem.at[c, 1])
        self.push(c, self.half(c, 0), HALF, p.me ^ 1, 5)
        self.push(c, self.half(c, 0), HALF, p.ring(d, 1), 2)
        self.push(c, self.half(c, 0), HALF, p.ring(d, 3), 3)

    def forward(self):
        p = self.p
        for side, t in ((0, 3), (1, 1)):
            for c in COLOURS:
                bytes_wait(self.g.at[c, pl.ds(0, HALF)], self.rsem.at[c, 2 + side])
                self.push(c, self.half(c, t), HALF, p.me ^ 1, 6 + 2 * side)
                self.push(c, self.half(c, t) + side * 8, 8, p.ring(DIMS[c][2], 4 - t), 4)

    def last(self):
        for c in COLOURS:
            bytes_wait(self.g.at[c, pl.ds(0, HALF)], self.rsem.at[c, 4])
            self.push(c, self.half(c, 2), HALF, self.p.me ^ 1, 7)

    def partner_wait(self, k):
        for c in COLOURS:
            bytes_wait(self.g.at[c, pl.ds(0, HALF)], self.rsem.at[c, k])

    def drain(self):
        for c in COLOURS:
            bytes_wait(self.g.at[c, pl.ds(0, 127)], self.ssem)


def load_rows(z_ref, xc_ref):
    def body(i, _):
        for r2 in PAIR:
            for p in QUAD:
                for core in PAIR:
                    at = p * PLANE + r2 * SIDE + core * HALF
                    xc_ref[i, pl.ds(at, HALF), :] = z_ref[i, pl.ds((p * SIDE + core) * 6 + r2, HALF, stride=12), :]
                    xc_ref[i, pl.ds(256 + at, HALF), :] = z_ref[i, pl.ds((p * 2 + core) * 6 + 2 + r2, HALF, stride=48), :]
                    for x in QUAD:
                        xc_ref[i, pl.ds(512 + at + x * 4, 4), :] = z_ref[i, pl.ds((p * 8 + x * 2 + core) * 6 + 4 + r2, 4, stride=192), :]
        return 0
    lax.fori_loop(0, z_ref.shape[0], body, 0)


def store_rows(place, y_ref, hb_ref, t):
    def body(i, _):
        p0, p1, p2 = (place.plane(c, t) for c in COLOURS)
        for r2 in PAIR:
            for core in PAIR:
                at = r2 * SIDE + core * HALF
                y_ref[i, pl.ds(p0 * 192 + core * 6 + r2, HALF, stride=12), :] = hb_ref[i, pl.ds(at, HALF), :]
                y_ref[i, pl.ds(p1 * 12 + core * 6 + 2 + r2, HALF, stride=48), :] = hb_ref[i, pl.ds(PLANE + at, HALF), :]
                for x in QUAD:
                    y_ref[i, pl.ds(p2 * 48 + x * 12 + core * 6 + 4 + r2, 4, stride=192), :] = hb_ref[i, pl.ds(128 + at + x * 4, 4), :]
        return 0
    lax.fori_loop(0, y_ref.shape[0], body, 0)


def inbox(c, place):
    x, y, z = place.at
    if c == 0:
        return place.me
    if c == 1:
        return x * SIDE + z * 8 + y * 2 + place.core
    return y * SIDE + z * 8 + x * 2 + place.core


def each_plane(place, rb_ref, esem, fn):
    def body(step, _):
        @pl.when(step == 0)
        def _():
            bytes_wait(rb_ref.at[:, pl.ds(0, 31)], esem.at[step])

        @pl.when(step > 0)
        def _():
            bytes_wait(rb_ref.at[:, pl.ds(0, SIDE)], esem.at[step])
        for c in COLOURS:
            q = place.plane(c, step)
            for g in QUAD:
                fn(c, q, g, rb_ref[c, pl.ds(mult(q * SIDE + g * 8, 8), 8)].reshape(96, 128))
        return 0
    lax.fori_loop(0, 4, body, 0)


def receive_rows(place, rb_ref, esem, um_ref, xc_ref):
    def put(c, q, g, x):
        f = dotf(um_ref[...], x)
        for b in PAIR:
            for r in range(6):
                for core in PAIR:
                    v = f[(b * 6 + r) * 8 + core * 4:(b * 6 + r) * 8 + core * 4 + 4]
                    at = (r % 2) * SIDE + core * HALF
                    if c == 1:
                        rows = (pl.ds(g * PLANE + at + q, 4, stride=4), pl.ds(mult(q * PLANE, PLANE) + 256 + at + g * 4, 4), pl.ds(512 + at + q * 4 + g, 4, stride=PLANE))
                    else:
                        zz, y = (q, g) if c == 0 else (g, q)
                        first = pl.ds(mult(q * PLANE, PLANE) + at + g * 4, 4) if c == 0 else pl.ds(g * PLANE + at + q * 4, 4)
                        rows = (first, pl.ds(256 + at + zz * 4 + y, 4, stride=PLANE), pl.ds(512 + at + y * PLANE + zz, 4, stride=4))
                    xc_ref[2 * c + b, rows[r // 2], :] = v
    each_plane(place, rb_ref, esem, put)


def finish_rows(place, rb_ref, esem, um1_ref, um2_ref, y_ref):
    def put(c, q, g, x):
        f = dotf(um1_ref[...] if c == 1 else um2_ref[...], x)
        for b in PAIR:
            for r in range(6):
                at = (b * 6 + r) * 8
                if c == 1:
                    for core in PAIR:
                        rows = pl.ds(g * 192 + q * 12 + core * 6 + r, 4, stride=48)
                        y_ref[2 * c + b, rows, :] = y_ref[2 * c + b, rows, :] + f[at + core * 4:at + core * 4 + 4]
                else:
                    rows = pl.ds((q * SIDE + g * 8) * 6 + r if c == 0 else (g * SIDE + q * 8) * 6 + r, 8, stride=6)
                    y_ref[2 * c + b, rows, :] = y_ref[2 * c + b, rows, :] + f[at:at + 8]
    each_plane(place, rb_ref, esem, put)


def stage(end, place, gather, heads, xc_ref, b_ref, gb_ref, w_ref, wb_ref, wo_ref, w1_ref, w2_ref, bm_ref, pm_ref, y_ref, rb_ref, esem, fsem,
          u_ref, q_ref, g_ref, kT_ref, v_ref, bf_ref, hb_ref, sb_ref, s_refs, p_refs, wkT_ref, entry_wait):
    per, n, c = xc_ref.shape
    hd = c // heads
    nq = n // 4
    scale = hd ** -0.5 * LOG2E
    me = place.me

    wb = wb_ref[...].astype(F32)
    none = jnp.zeros_like(wb)
    wide = [jnp.concatenate(p, axis=0).astype(BF16) for p in ((wb, none), (none, wb))]

    def bias_rows(col, _):
        acc = None
        for r2 in PAIR:
            i = col * 2 + r2
            u = ln(xc_ref[i])
            u_ref[i] = u
            t = dot_nt(wide[r2], u)
            acc = t if acc is None else acc + t
        b_ref[col] = acc.astype(BF16)
        for k in COLOURS:
            @pl.when(col == k)
            def _():
                if k == 0 and not end:
                    entry_wait()
                gather.first(k)
        return 0
    lax.fori_loop(0, 3, bias_rows, 0)

    wkT_ref[...] = w_ref[:, c:2 * c].T

    def project(i):
        u = u_ref[i]
        kT_ref[i] = dot_nt(wkT_ref[...], u).astype(BF16)
        q_ref[i] = dotf(u, w_ref[:, :c]).astype(BF16)
        vg = dotf(u, w_ref[:, 2 * c:])
        v_ref[i, :, :c] = vg[:, :c].astype(BF16)
        if not end:
            v_ref[i, :, c:] = jnp.ones((n, c), BF16)
        g_ref[i] = jax.nn.sigmoid(vg[:, c:])

    def prepare(i, _):
        project(i)
        for col in COLOURS:
            @pl.when(i == col)
            def _():
                gather.second(col)

            @pl.when(i == col + 3)
            def _():
                gather.third(col)
        return 0
    lax.fori_loop(0, per, prepare, 0)

    order = (0, 3, 2, 1)

    def pick(step):
        return lax.rem(4 - step, 4)

    def send(col, plane, o, step):
        k = lax.rem(slot_of(col, place), SIDE) ^ o
        rcopy(sb_ref.at[col, plane * SIDE + k], rb_ref.at[col, inbox(col, place)], fsem, esem.at[step], dest_of(col, plane, k)).start()

    def finish_block(t):
        if not end:
            store_rows(place, y_ref, hb_ref, t)

    def block(step, _):
        first = isinstance(step, int)
        t = 0 if first else pick(step)
        before = None if first else [place.plane(col, pick(step - 1)) for col in COLOURS]
        gather.partner_wait(5 + step)
        planes = [place.plane(col, t) for col in COLOURS]
        for col in COLOURS:
            b = gb_ref[col, pl.ds(mult(planes[col] * SIDE, SIDE), SIDE)].reshape(256, n)
            f = dotf(bm_ref[...], b) * LOG2E
            for h in range(heads):
                bf_ref[h * nq + col * PLANE:h * nq + (col + 1) * PLANE, :] = f[h * PLANE:(h + 1) * PLANE]
        rows = [pl.ds(mult(col * 256 + planes[col] * PLANE, PLANE), PLANE) for col in COLOURS]

        lane = lax.broadcasted_iota(jnp.int32, (nq, c), 1) // hd

        def scores(i):
            qb = jnp.concatenate([q_ref[i, r, :] for r in rows], axis=0)
            qm = jnp.concatenate([jnp.where(lane == h, qb, jnp.zeros_like(qb)) for h in range(heads)], axis=0)
            s_refs[i % 2][...] = dotf(qm, kT_ref[i]) * scale + bf_ref[...]

        def mix(i):
            t = s_refs[i % 2][...]
            m = jnp.max(t, axis=-1, keepdims=True)
            o = dotf(jnp.exp2(t - m).astype(BF16), v_ref[i])
            o = o[:, :c] / o[:, c:]
            res = jnp.zeros((nq, c), F32)
            for h in range(heads):
                res = jnp.where(lane == h, o[h * nq:(h + 1) * nq], res)
            og = (res * jnp.concatenate([g_ref[i, r, :] for r in rows], axis=0)).astype(BF16)
            upd = dotf(og, wo_ref[...])
            if end:
                hb_ref[i] = upd
            else:
                hb_ref[i] = jnp.concatenate([xc_ref[i, r, :] for r in rows], axis=0) + upd

        if not first:
            @pl.when(step > 1)
            def _():
                for col in COLOURS:
                    send(col, before[col], 0, step - 1)
        scores(0)
        for i in range(per):
            if not first:
                for o in range(1 + i * 31 // per, 1 + (i + 1) * 31 // per):
                    for col in COLOURS:
                        send(col, before[col], o, step - 1)
            if i + 1 < per:
                scores(i + 1)
            mix(i)
        if first:
            gather.forward()
        else:
            @pl.when(step == 1)
            def _():
                gather.last()

        if end:
            def trans(i, _):
                upd = jnp.concatenate([hb_ref[2 * i], hb_ref[2 * i + 1]], axis=0)
                two = jnp.concatenate([xc_ref[2 * i + a, r, :] for a in PAIR for r in rows], axis=0) + upd
                hid = jnp.maximum(dotf(ln(two), w1_ref[...]), 0).astype(BF16)
                new = upd + dotf(hid, w2_ref[...])
                hb_ref[2 * i] = new[:nq]
                hb_ref[2 * i + 1] = new[nq:]
                return 0
            lax.fori_loop(0, per // 2, trans, 0, unroll=3)
        def pack(kg, _):
            for col in COLOURS:
                x = jnp.concatenate([hb_ref[i, pl.ds(mult(col * PLANE + r2 * SIDE + kg * 8, 8), 8), :] for i in range(per) for r2 in PAIR], axis=0)
                f = dotf(pm_ref[...], x.astype(BF16)).reshape(8, 12, c).astype(BF16)
                sb_ref[col, pl.ds(mult(planes[col] * SIDE + kg * 8, 8), 8)] = f
            return 0
        lax.fori_loop(0, 4, pack, 0, unroll=4)
        if first:
            finish_block(0)
        else:
            @pl.when(step < 3)
            def _():
                finish_block(t)

        return 0

    block(0, 0)
    lax.fori_loop(1, 4, block, 0)
    tail = [place.plane(col, order[3]) for col in COLOURS]

    def send_tail(o, _):
        for col in COLOURS:
            send(col, tail[col], o, 3)
        return 0
    lax.fori_loop(0, SIDE, send_tail, 0)
    finish_block(order[3])
    for col in COLOURS:
        rb_ref[col, inbox(col, place)] = sb_ref[col, slot_of(col, place)]


def drain(gather, rb_ref, fsem):
    gather.drain()
    bytes_wait(rb_ref.at[:, pl.ds(0, 127)], fsem)


def kernel(heads, devs, z_ref, ws_ref, wbs_ref, wos_ref, we_ref, wbe_ref, woe_ref, w1_ref, w2_ref, bm_ref, pm_ref, um1_ref, um2_ref, y_ref,
           xc_ref, b_ref, gb1_ref, gb2_ref, rb1_ref, rb2_ref, u_ref, q_ref, g_ref, kT_ref, v_ref, bf_ref, hb_ref, sb_ref, sa_ref, sb2_ref, pa_ref, pb_ref, wkT_ref,
           gs1, gr1, gs2, gr2, e1, f1, e2, f2):
    place = Place()
    barrier = pltpu.get_barrier_semaphore()

    friends = [place.me ^ 1] + [place.ring(d, t) for d in COLOURS for t in QUAD if t]
    for peer in friends:
        pl.semaphore_signal(barrier, inc=1, device_id={'sp': peer}, device_id_type=MESH)

    def entry_wait():
        pl.semaphore_wait(barrier, len(friends))
    work = (u_ref, q_ref, g_ref, kT_ref, v_ref, bf_ref, hb_ref, sb_ref, (sa_ref, sb2_ref), (pa_ref, pb_ref), wkT_ref, entry_wait)
    load_rows(z_ref, xc_ref)
    gather = Gather(place, b_ref.at[0], gb1_ref, gs1, gr1)
    stage(False, place, gather, heads, xc_ref, b_ref.at[0], gb1_ref, ws_ref, wbs_ref, wos_ref, w1_ref, w2_ref,
          bm_ref, pm_ref, y_ref, rb1_ref, e1, f1, *work)
    receive_rows(place, rb1_ref, e1, um1_ref, xc_ref)
    drain(gather, rb1_ref, f1)
    gather = Gather(place, b_ref.at[1], gb2_ref, gs2, gr2)
    stage(True, place, gather, heads, xc_ref, b_ref.at[1], gb2_ref, we_ref, wbe_ref, woe_ref, w1_ref, w2_ref,
          bm_ref, pm_ref, y_ref, rb2_ref, e2, f2, *work)
    finish_rows(place, rb2_ref, e2, um1_ref, um2_ref, y_ref)
    drain(gather, rb2_ref, f2)


def pack_matrix():
    m = np.zeros((8, 12, 6, 2, 8), np.float32)
    for k in range(8):
        for i in range(6):
            for r in PAIR:
                m[k, i * 2 + r, i, r, k] = 1
    return jnp.asarray(m.reshape(96, 96), BF16)


def unpack_matrix(swap):
    m = np.zeros((2, 6, 8, 8, 12), np.float32)
    for k in range(8):
        for i in range(6):
            for r in PAIR:
                row = (k % 2) * 4 + k // 2 if swap else k
                m[r, i, row, k, i * 2 + r] = 1
    return jnp.asarray(m.reshape(96, 96), BF16)


def bias_matrix(heads):
    m = np.zeros((heads, 2, SIDE, SIDE, 2, heads), np.float32)
    for k in range(SIDE):
        for r in PAIR:
            for h in range(heads):
                m[h, r, k, k, r, h] = 1
    return jnp.asarray(m.reshape(256, 256), BF16)


def solution(mesh):
    devs = mesh.shape['sp']
    row_spec = P(('dp', 'sp'), None, None)
    vmem = pl.BlockSpec(memory_space=pltpu.VMEM)
    dma = pltpu.SemaphoreType.DMA

    def local_fn(z, wqkvg_s, wb_s, wo_s, wqkvg_e, wb_e, wo_e, w1, w2):
        per, n, c = z.shape
        heads = wb_s.shape[0]
        args = (z, wqkvg_s, wb_s, wo_s, wqkvg_e, wb_e, wo_e, w1, w2, bias_matrix(heads), pack_matrix(), unpack_matrix(True), unpack_matrix(False))
        return pl.pallas_call(
            functools.partial(kernel, heads, devs), in_specs=[vmem] * len(args), out_specs=vmem,
            out_shape=jax.ShapeDtypeStruct(z.shape, F32),
            scratch_shapes=[
                pltpu.VMEM((per, n, c), F32), pltpu.VMEM((2, 3, 8, n), BF16),
                pltpu.VMEM((3, devs, 8, n), BF16), pltpu.VMEM((3, devs, 8, n), BF16),
                pltpu.VMEM((3, devs, 12, c), BF16), pltpu.VMEM((3, devs, 12, c), BF16),
                pltpu.VMEM((per, n, c), BF16), pltpu.VMEM((per, n, c), BF16), pltpu.VMEM((per, n, c), F32),
                pltpu.VMEM((per, c, n), BF16), pltpu.VMEM((per, n, 2 * c), BF16), pltpu.VMEM((heads * n // 4, n), F32),
                pltpu.VMEM((per, n // 4, c), F32), pltpu.VMEM((3, devs, 12, c), BF16),
                pltpu.VMEM((heads * n // 4, n), F32), pltpu.VMEM((heads * n // 4, n), F32),
                pltpu.VMEM((heads * n // 4, n), BF16), pltpu.VMEM((heads * n // 4, n), BF16),
                pltpu.VMEM((c, c), BF16),
                dma, dma((3, 9)), dma, dma((3, 9)), dma((4,)), dma, dma((4,)), dma],
            compiler_params=pltpu.CompilerParams(has_side_effects=True, collective_id=0, vmem_limit_bytes=60 * 2**20), name='block')(*args)

    return jax.shard_map(local_fn, mesh=mesh, in_specs=(row_spec,) + (P(),) * 8, out_specs=row_spec, check_vma=False)
```

```python
import functools
import math
import jax
import jax.numpy as jnp
import numpy as np
from jax import lax
from jax.experimental import pallas as pl
from jax.experimental.pallas import tpu as pltpu
from jax.sharding import PartitionSpec as P

F32, BF16 = jnp.float32, jnp.bfloat16
MESH = pl.DeviceIdType.MESH
LOG2E = math.log2(math.e)
EPS = 1e-5
X, Y, Z = 0, 1, 2
COLOURS = range(3)
PAIR = range(2)
QUAD = range(4)
HALF, SIDE, PLANE = 16, 32, 64
DEV = (2, 8, 32)
DIMS = ((X, Y, Z), (Y, Z, X), (Z, X, Y))
SLOT = ((1, 4, 32), (32, 1, 4), (4, 32, 1))


def ln(x):
    mu = jnp.mean(x, axis=-1, keepdims=True)
    c = x - mu
    var = jnp.mean(c * c, axis=-1, keepdims=True)
    return (c * lax.rsqrt(var + EPS)).astype(BF16)


def dotf(a, b):
    return jnp.dot(a, b, preferred_element_type=F32)


def dot_nt(a, b):
    return lax.dot_general(a, b, (((1,), (1,)), ((), ())), preferred_element_type=F32)


def mult(v, k):
    return pl.multiple_of(v, k)


def rcopy(src, dst, ssem, rsem, peer):
    return pltpu.make_async_remote_copy(src_ref=src, dst_ref=dst, send_sem=ssem, recv_sem=rsem, device_id={'sp': peer}, device_id_type=MESH)


def bytes_wait(ref, sem):
    pltpu.make_async_copy(ref, ref, sem).wait()


class Place:
    def __init__(self):
        self.me = lax.axis_index('sp')
        self.core = lax.rem(self.me, 2)
        self.at = [lax.rem(self.me // s, 4) for s in DEV]

    def ring(self, dim, t):
        return self.me + (lax.rem(self.at[dim] + t, 4) - self.at[dim]) * DEV[dim]

    def plane(self, c, t):
        return lax.rem(self.at[DIMS[c][2]] + t, 4)


def slot_of(c, place):
    return place.core * HALF + sum(place.at[d] * SLOT[c][d] for d in COLOURS)


def dest_of(c, plane, k):
    if c == 0:
        return plane * SIDE + lax.rem(k, HALF) * 2 + k // HALF
    if c == 1:
        return lax.rem(k, HALF) * 8 + plane * 2 + k // HALF
    return lax.rem(k, 4) * SIDE + plane * 8 + lax.rem(k // 4, 4) * 2 + k // HALF


class Gather:
    def __init__(self, place, b_ref, g_ref, ssem, rsem):
        self.p, self.b, self.g, self.ssem, self.rsem = place, b_ref, g_ref, ssem, rsem

    def push(self, c, start, count, peer, k):
        part = self.g.at[c, pl.ds(start, count)]
        rcopy(part, part, self.ssem, self.rsem.at[c, k], peer).start()

    def half(self, c, t):
        return self.p.plane(c, t) * SIDE + self.p.core * HALF

    def first(self, c):
        p = self.p
        slot = slot_of(c, p)
        for t in (1, 3, 2):
            rcopy(self.b.at[c], self.g.at[c, slot], self.ssem, self.rsem.at[c, 0], p.ring(DIMS[c][0], t)).start()
        self.g[c, slot] = self.b[c]

    def second(self, c):
        p = self.p
        b = DIMS[c][1]
        bytes_wait(self.g.at[c, pl.ds(0, 3)], self.rsem.at[c, 0])
        for t in (1, 3, 2):
            self.push(c, self.half(c, 0) + p.at[b] * 4, 4, p.ring(b, t), 1)

    def third(self, c):
        p = self.p
        d = DIMS[c][2]
        bytes_wait(self.g.at[c, pl.ds(0, 12)], self.rsem.at[c, 1])
        self.push(c, self.half(c, 0), HALF, p.me ^ 1, 5)
        self.push(c, self.half(c, 0), HALF, p.ring(d, 1), 2)
        self.push(c, self.half(c, 0), HALF, p.ring(d, 3), 3)

    def forward(self):
        p = self.p
        for side, t in ((0, 3), (1, 1)):
            for c in COLOURS:
                bytes_wait(self.g.at[c, pl.ds(0, HALF)], self.rsem.at[c, 2 + side])
                self.push(c, self.half(c, t), HALF, p.me ^ 1, 6 + 2 * side)
                self.push(c, self.half(c, t) + side * 8, 8, p.ring(DIMS[c][2], 4 - t), 4)

    def last(self):
        for c in COLOURS:
            bytes_wait(self.g.at[c, pl.ds(0, HALF)], self.rsem.at[c, 4])
            self.push(c, self.half(c, 2), HALF, self.p.me ^ 1, 7)

    def partner_wait(self, k):
        for c in COLOURS:
            bytes_wait(self.g.at[c, pl.ds(0, HALF)], self.rsem.at[c, k])

    def drain(self):
        for c in COLOURS:
            bytes_wait(self.g.at[c, pl.ds(0, 127)], self.ssem)


def load_rows(z_ref, xc_ref):
    def body(i, _):
        for r2 in PAIR:
            for p in QUAD:
                for core in PAIR:
                    at = p * PLANE + r2 * SIDE + core * HALF
                    xc_ref[i, pl.ds(at, HALF), :] = z_ref[i, pl.ds((p * SIDE + core) * 6 + r2, HALF, stride=12), :]
                    xc_ref[i, pl.ds(256 + at, HALF), :] = z_ref[i, pl.ds((p * 2 + core) * 6 + 2 + r2, HALF, stride=48), :]
                    for x in QUAD:
                        xc_ref[i, pl.ds(512 + at + x * 4, 4), :] = z_ref[i, pl.ds((p * 8 + x * 2 + core) * 6 + 4 + r2, 4, stride=192), :]
        return 0
    lax.fori_loop(0, z_ref.shape[0], body, 0)


def store_rows(place, y_ref, hb_ref, t):
    def body(i, _):
        p0, p1, p2 = (place.plane(c, t) for c in COLOURS)
        for r2 in PAIR:
            for core in PAIR:
                at = r2 * SIDE + core * HALF
                y_ref[i, pl.ds(p0 * 192 + core * 6 + r2, HALF, stride=12), :] = hb_ref[i, pl.ds(at, HALF), :]
                y_ref[i, pl.ds(p1 * 12 + core * 6 + 2 + r2, HALF, stride=48), :] = hb_ref[i, pl.ds(PLANE + at, HALF), :]
                for x in QUAD:
                    y_ref[i, pl.ds(p2 * 48 + x * 12 + core * 6 + 4 + r2, 4, stride=192), :] = hb_ref[i, pl.ds(128 + at + x * 4, 4), :]
        return 0
    lax.fori_loop(0, y_ref.shape[0], body, 0)


def inbox(c, place):
    x, y, z = place.at
    if c == 0:
        return place.me
    if c == 1:
        return x * SIDE + z * 8 + y * 2 + place.core
    return y * SIDE + z * 8 + x * 2 + place.core


def take_plane(place, rb_ref, c, step, fn):
    q = place.plane(c, step)
    for g in QUAD:
        fn(c, q, g, rb_ref[c, pl.ds(mult(q * SIDE + g * 8, 8), 8)].reshape(96, 128))


def early_planes(place, rb_ref, esem, fn):
    def body(step, _):
        for c in COLOURS:
            @pl.when(step == 0)
            def _():
                bytes_wait(rb_ref.at[c, pl.ds(0, SIDE - 1)], esem.at[step, c])

            @pl.when(step > 0)
            def _():
                bytes_wait(rb_ref.at[c, pl.ds(0, SIDE)], esem.at[step, c])
        for c in COLOURS:
            take_plane(place, rb_ref, c, step, fn)
        return 0
    lax.fori_loop(0, 3, body, 0)


def last_plane(place, rb_ref, esem, c, fn):
    bytes_wait(rb_ref.at[c, pl.ds(0, SIDE)], esem.at[3, c])
    take_plane(place, rb_ref, c, 3, fn)


def receiver(um_ref, xc_ref):
    def put(c, q, g, x):
        f = dotf(um_ref[...], x)
        for b in PAIR:
            for r in range(6):
                for core in PAIR:
                    v = f[(b * 6 + r) * 8 + core * 4:(b * 6 + r) * 8 + core * 4 + 4]
                    at = (r % 2) * SIDE + core * HALF
                    if c == 1:
                        rows = (pl.ds(g * PLANE + at + q, 4, stride=4), pl.ds(mult(q * PLANE, PLANE) + 256 + at + g * 4, 4), pl.ds(512 + at + q * 4 + g, 4, stride=PLANE))
                    else:
                        zz, y = (q, g) if c == 0 else (g, q)
                        first = pl.ds(mult(q * PLANE, PLANE) + at + g * 4, 4) if c == 0 else pl.ds(g * PLANE + at + q * 4, 4)
                        rows = (first, pl.ds(256 + at + zz * 4 + y, 4, stride=PLANE), pl.ds(512 + at + y * PLANE + zz, 4, stride=4))
                    xc_ref[2 * c + b, rows[r // 2], :] = v
    return put


def finisher(um1_ref, um2_ref, y_ref):
    def put(c, q, g, x):
        f = dotf(um1_ref[...] if c == 1 else um2_ref[...], x)
        for b in PAIR:
            for r in range(6):
                at = (b * 6 + r) * 8
                if c == 1:
                    for core in PAIR:
                        rows = pl.ds(g * 192 + q * 12 + core * 6 + r, 4, stride=48)
                        y_ref[2 * c + b, rows, :] = y_ref[2 * c + b, rows, :] + f[at + core * 4:at + core * 4 + 4]
                else:
                    rows = pl.ds((q * SIDE + g * 8) * 6 + r if c == 0 else (g * SIDE + q * 8) * 6 + r, 8, stride=6)
                    y_ref[2 * c + b, rows, :] = y_ref[2 * c + b, rows, :] + f[at:at + 8]
    return put


def stage(end, place, gather, heads, xc_ref, b_ref, gb_ref, w_ref, wb_ref, wo_ref, w1_ref, w2_ref, bm_ref, pm_ref, y_ref, rb_ref, esem, fsem,
          u_ref, q_ref, g_ref, kT_ref, v_ref, bf_ref, hb_ref, sb_ref, s_refs, p_refs, wkT_ref, entry_wait, arrive, settle):
    per, n, c = xc_ref.shape
    hd = c // heads
    nq = n // 4
    scale = hd ** -0.5 * LOG2E
    me = place.me

    wb = wb_ref[...].astype(F32)
    none = jnp.zeros_like(wb)
    wide = [jnp.concatenate(p, axis=0).astype(BF16) for p in ((wb, none), (none, wb))]

    def bias_rows(col, _):
        for k in COLOURS:
            @pl.when(col == k)
            def _():
                arrive(k)
        acc = None
        for r2 in PAIR:
            i = col * 2 + r2
            u = ln(xc_ref[i])
            u_ref[i] = u
            t = dot_nt(wide[r2], u)
            acc = t if acc is None else acc + t
        b_ref[col] = acc.astype(BF16)
        for k in COLOURS:
            @pl.when(col == k)
            def _():
                if k == 0 and not end:
                    entry_wait()
                gather.first(k)
        return 0
    lax.fori_loop(0, 3, bias_rows, 0)

    wkT_ref[...] = w_ref[:, c:2 * c].T

    def project(i):
        u = u_ref[i]
        kT_ref[i] = dot_nt(wkT_ref[...], u).astype(BF16)
        q_ref[i] = dotf(u, w_ref[:, :c]).astype(BF16)
        vg = dotf(u, w_ref[:, 2 * c:])
        v_ref[i, :, :c] = vg[:, :c].astype(BF16)
        if not end:
            v_ref[i, :, c:] = jnp.ones((n, c), BF16)
        g_ref[i] = jax.nn.sigmoid(vg[:, c:])

    def prepare(i, _):
        project(i)
        for col in COLOURS:
            @pl.when(i == col)
            def _():
                gather.second(col)

            @pl.when(i == col + 3)
            def _():
                gather.third(col)
        return 0
    lax.fori_loop(0, per, prepare, 0)

    settle()
    order = (0, 3, 2, 1)

    def pick(step):
        return lax.rem(4 - step, 4)

    def send(col, plane, o, step):
        k = lax.rem(slot_of(col, place), SIDE) ^ o
        rcopy(sb_ref.at[col, plane * SIDE + k], rb_ref.at[col, inbox(col, place)], fsem, esem.at[step, col], dest_of(col, plane, k)).start()

    def finish_block(t):
        if not end:
            store_rows(place, y_ref, hb_ref, t)

    def block(step, _):
        first = isinstance(step, int)
        t = 0 if first else pick(step)
        before = None if first else [place.plane(col, pick(step - 1)) for col in COLOURS]
        gather.partner_wait(5 + step)
        planes = [place.plane(col, t) for col in COLOURS]
        for col in COLOURS:
            b = gb_ref[col, pl.ds(mult(planes[col] * SIDE, SIDE), SIDE)].reshape(256, n)
            f = dotf(bm_ref[...], b) * LOG2E
            for h in range(heads):
                bf_ref[h * nq + col * PLANE:h * nq + (col + 1) * PLANE, :] = f[h * PLANE:(h + 1) * PLANE]
        rows = [pl.ds(mult(col * 256 + planes[col] * PLANE, PLANE), PLANE) for col in COLOURS]

        lane = lax.broadcasted_iota(jnp.int32, (nq, c), 1) // hd

        def scores(i):
            qb = jnp.concatenate([q_ref[i, r, :] for r in rows], axis=0)
            qm = jnp.concatenate([jnp.where(lane == h, qb, jnp.zeros_like(qb)) for h in range(heads)], axis=0)
            s_refs[i % 2][...] = dotf(qm, kT_ref[i]) * scale + bf_ref[...]

        def mix(i):
            t = s_refs[i % 2][...]
            m = jnp.max(t, axis=-1, keepdims=True)
            o = dotf(jnp.exp2(t - m).astype(BF16), v_ref[i])
            o = o[:, :c] / o[:, c:]
            res = jnp.zeros((nq, c), F32)
            for h in range(heads):
                res = jnp.where(lane == h, o[h * nq:(h + 1) * nq], res)
            og = (res * jnp.concatenate([g_ref[i, r, :] for r in rows], axis=0)).astype(BF16)
            upd = dotf(og, wo_ref[...])
            if end:
                hb_ref[i] = upd
            else:
                hb_ref[i] = jnp.concatenate([xc_ref[i, r, :] for r in rows], axis=0) + upd

        if not first:
            @pl.when(step > 1)
            def _():
                for col in COLOURS:
                    send(col, before[col], 0, step - 1)
        scores(0)
        for i in range(per):
            if not first:
                for o in range(1 + i * 31 // per, 1 + (i + 1) * 31 // per):
                    for col in COLOURS:
                        send(col, before[col], o, step - 1)
            if i + 1 < per:
                scores(i + 1)
            mix(i)
        if first:
            gather.forward()
        else:
            @pl.when(step == 1)
            def _():
                gather.last()

        if end:
            def trans(i, _):
                upd = jnp.concatenate([hb_ref[2 * i], hb_ref[2 * i + 1]], axis=0)
                two = jnp.concatenate([xc_ref[2 * i + a, r, :] for a in PAIR for r in rows], axis=0) + upd
                hid = jnp.maximum(dotf(ln(two), w1_ref[...]), 0).astype(BF16)
                new = upd + dotf(hid, w2_ref[...])
                hb_ref[2 * i] = new[:nq]
                hb_ref[2 * i + 1] = new[nq:]
                return 0
            lax.fori_loop(0, per // 2, trans, 0, unroll=3)
        def pack(kg, _):
            for col in COLOURS:
                x = jnp.concatenate([hb_ref[i, pl.ds(mult(col * PLANE + r2 * SIDE + kg * 8, 8), 8), :] for i in range(per) for r2 in PAIR], axis=0)
                f = dotf(pm_ref[...], x.astype(BF16)).reshape(8, 12, c).astype(BF16)
                sb_ref[col, pl.ds(mult(planes[col] * SIDE + kg * 8, 8), 8)] = f
            return 0
        lax.fori_loop(0, 4, pack, 0, unroll=4)
        if first:
            finish_block(0)
        else:
            @pl.when(step < 3)
            def _():
                finish_block(t)

        return 0

    block(0, 0)
    lax.fori_loop(1, 4, block, 0)
    tail = [place.plane(col, order[3]) for col in COLOURS]

    for col in COLOURS:
        def send_tail(o, _):
            send(col, tail[col], o, 3)
            return 0
        lax.fori_loop(0, SIDE, send_tail, 0)
    finish_block(order[3])
    for col in COLOURS:
        rb_ref[col, inbox(col, place)] = sb_ref[col, slot_of(col, place)]


def drain(gather, rb_ref, fsem):
    gather.drain()
    bytes_wait(rb_ref.at[:, pl.ds(0, 127)], fsem)


def kernel(heads, devs, z_ref, ws_ref, wbs_ref, wos_ref, we_ref, wbe_ref, woe_ref, w1_ref, w2_ref, bm_ref, pm_ref, um1_ref, um2_ref, y_ref,
           xc_ref, b_ref, gb1_ref, gb2_ref, rb1_ref, rb2_ref, u_ref, q_ref, g_ref, kT_ref, v_ref, bf_ref, hb_ref, sb_ref, sa_ref, sb2_ref, pa_ref, pb_ref, wkT_ref,
           gs1, gr1, gs2, gr2, e1, f1, e2, f2):
    place = Place()
    barrier = pltpu.get_barrier_semaphore()

    friends = [place.me ^ 1] + [place.ring(d, t) for d in COLOURS for t in QUAD if t]
    for peer in friends:
        pl.semaphore_signal(barrier, inc=1, device_id={'sp': peer}, device_id_type=MESH)

    def entry_wait():
        pl.semaphore_wait(barrier, len(friends))
    work = (u_ref, q_ref, g_ref, kT_ref, v_ref, bf_ref, hb_ref, sb_ref, (sa_ref, sb2_ref), (pa_ref, pb_ref), wkT_ref, entry_wait)
    load_rows(z_ref, xc_ref)
    gather = Gather(place, b_ref.at[0], gb1_ref, gs1, gr1)
    nothing = lambda *_: None
    stage(False, place, gather, heads, xc_ref, b_ref.at[0], gb1_ref, ws_ref, wbs_ref, wos_ref, w1_ref, w2_ref,
          bm_ref, pm_ref, y_ref, rb1_ref, e1, f1, *work, nothing, nothing)
    put = receiver(um1_ref, xc_ref)
    early_planes(place, rb1_ref, e1, put)
    gather2 = Gather(place, b_ref.at[1], gb2_ref, gs2, gr2)
    stage(True, place, gather2, heads, xc_ref, b_ref.at[1], gb2_ref, we_ref, wbe_ref, woe_ref, w1_ref, w2_ref,
          bm_ref, pm_ref, y_ref, rb2_ref, e2, f2, *work,
          lambda c: last_plane(place, rb1_ref, e1, c, put), lambda: drain(gather, rb1_ref, f1))
    put2 = finisher(um1_ref, um2_ref, y_ref)
    early_planes(place, rb2_ref, e2, put2)
    for c in COLOURS:
        last_plane(place, rb2_ref, e2, c, put2)
    drain(gather2, rb2_ref, f2)


def pack_matrix():
    m = np.zeros((8, 12, 6, 2, 8), np.float32)
    for k in range(8):
        for i in range(6):
            for r in PAIR:
                m[k, i * 2 + r, i, r, k] = 1
    return jnp.asarray(m.reshape(96, 96), BF16)


def unpack_matrix(swap):
    m = np.zeros((2, 6, 8, 8, 12), np.float32)
    for k in range(8):
        for i in range(6):
            for r in PAIR:
                row = (k % 2) * 4 + k // 2 if swap else k
                m[r, i, row, k, i * 2 + r] = 1
    return jnp.asarray(m.reshape(96, 96), BF16)


def bias_matrix(heads):
    m = np.zeros((heads, 2, SIDE, SIDE, 2, heads), np.float32)
    for k in range(SIDE):
        for r in PAIR:
            for h in range(heads):
                m[h, r, k, k, r, h] = 1
    return jnp.asarray(m.reshape(256, 256), BF16)


def solution(mesh):
    devs = mesh.shape['sp']
    row_spec = P(('dp', 'sp'), None, None)
    vmem = pl.BlockSpec(memory_space=pltpu.VMEM)
    dma = pltpu.SemaphoreType.DMA

    def local_fn(z, wqkvg_s, wb_s, wo_s, wqkvg_e, wb_e, wo_e, w1, w2):
        per, n, c = z.shape
        heads = wb_s.shape[0]
        args = (z, wqkvg_s, wb_s, wo_s, wqkvg_e, wb_e, wo_e, w1, w2, bias_matrix(heads), pack_matrix(), unpack_matrix(True), unpack_matrix(False))
        return pl.pallas_call(
            functools.partial(kernel, heads, devs), in_specs=[vmem] * len(args), out_specs=vmem,
            out_shape=jax.ShapeDtypeStruct(z.shape, F32),
            scratch_shapes=[
                pltpu.VMEM((per, n, c), F32), pltpu.VMEM((2, 3, 8, n), BF16),
                pltpu.VMEM((3, devs, 8, n), BF16), pltpu.VMEM((3, devs, 8, n), BF16),
                pltpu.VMEM((3, devs, 12, c), BF16), pltpu.VMEM((3, devs, 12, c), BF16),
                pltpu.VMEM((per, n, c), BF16), pltpu.VMEM((per, n, c), BF16), pltpu.VMEM((per, n, c), F32),
                pltpu.VMEM((per, c, n), BF16), pltpu.VMEM((per, n, 2 * c), BF16), pltpu.VMEM((heads * n // 4, n), F32),
                pltpu.VMEM((per, n // 4, c), F32), pltpu.VMEM((3, devs, 12, c), BF16),
                pltpu.VMEM((heads * n // 4, n), F32), pltpu.VMEM((heads * n // 4, n), F32),
                pltpu.VMEM((heads * n // 4, n), BF16), pltpu.VMEM((heads * n // 4, n), BF16),
                pltpu.VMEM((c, c), BF16),
                dma, dma((3, 9)), dma, dma((3, 9)), dma((4, 3)), dma, dma((4, 3)), dma],
            compiler_params=pltpu.CompilerParams(has_side_effects=True, collective_id=0, vmem_limit_bytes=60 * 2**20), name='block')(*args)

    return jax.shard_map(local_fn, mesh=mesh, in_specs=(row_spec,) + (P(),) * 8, out_specs=row_spec, check_vma=False)
```
